16 devices in a mesh: dp: 2 (over y, z), sp: 8 (over x, core).
Axes of the slice: x: 4, y: 2, z: 1, core: 2. Of those that a mesh axis runs over, the one named last changes fastest.
The devices are a block of a 4x4x8 slice.
Arguments:
- latents: bfloat16 [8, 8, 576, 1152], P('dp', 'sp'), parts along dimension 0
- text_ctx: bfloat16 [8, 200, 1152], P('dp'), parts along dimension 0
- modulation: float32 [8, 6, 1152], P('dp'), parts along dimension 0
- pos_temporal: float32 [8, 1152], replicated
- w_qkv_spatial: bfloat16 [3, 16, 72, 1152], replicated
- w_out_spatial: bfloat16 [16, 72, 1152], replicated
- w_qkv_temporal: bfloat16 [3, 16, 72, 1152], replicated
- w_out_temporal: bfloat16 [16, 72, 1152], replicated
- w_query_cross: bfloat16 [16, 72, 1152], replicated
- w_kv_cross: bfloat16 [2, 16, 72, 1152], replicated
- w_out_cross: bfloat16 [16, 72, 1152], replicated
- w_mlp_in: bfloat16 [1152, 4608], replicated
- w_mlp_out: bfloat16 [4608, 1152], replicated
Outputs:
- output: bfloat16 [8, 8, 576, 1152], P('dp', 'sp'), parts along dimension 0
There are 2 independent parts. The reference program is written for one: setup_inputs(seed, part) draws one part's arguments, and reference() takes and returns one part's arrays. A program takes and returns all parts, laid end to end along the dimension named above; an argument that names none is the same for every part.
All inputs are finite; a program needn't handle non-finite values.
Results may differ from the reference program's by a relative error of at most 0.0150305.
Values are sent between devices in bfloat16 or wider.
A program may use at most 768 MiB of HBM per device.

```python
import jax
import jax.numpy as jnp
from jax import lax

BATCH_SIZE = 4
NUM_FRAMES = 8
NUM_PATCHES = 576
MODEL_WIDTH = 1152
NUM_HEADS = 16
TEXT_LEN = 200

HEAD_DIM = MODEL_WIDTH // NUM_HEADS
LN_EPS = 1e-6


def weight_draw(rng_key, arr_shape, fan_in):
    return (jax.random.normal(rng_key, arr_shape, jnp.float32) * (fan_in ** -0.5)).astype(jnp.bfloat16)


def setup_inputs(seed: int = 0, part: int = 0) -> dict:
    part_keys = jax.random.split(jax.random.fold_in(jax.random.key(seed), part), 6)
    shared_keys = jax.random.split(jax.random.key(seed + 1), 11)
    act_shape = (BATCH_SIZE, NUM_FRAMES, NUM_PATCHES, MODEL_WIDTH)
    token_base = jax.random.normal(part_keys[0], (BATCH_SIZE, 1, NUM_PATCHES, MODEL_WIDTH), jnp.float32)
    frame_base = jax.random.normal(part_keys[1], (BATCH_SIZE, NUM_FRAMES, 1, MODEL_WIDTH), jnp.float32)
    noise_part = jax.random.normal(part_keys[2], act_shape, jnp.float32)
    latents = (0.5 * token_base + 0.5 * frame_base + 0.6 * noise_part).astype(jnp.bfloat16)
    ctx_common = jax.random.normal(part_keys[3], (BATCH_SIZE, 1, MODEL_WIDTH), jnp.float32)
    ctx_noise = jax.random.normal(part_keys[4], (BATCH_SIZE, TEXT_LEN, MODEL_WIDTH), jnp.float32)
    text_ctx = (0.5 * ctx_common + ctx_noise).astype(jnp.bfloat16)
    gate_offset = jnp.array([0.0, 0.0, 1.0, 0.0, 0.0, 1.0], jnp.float32)[None, :, None]
    modulation = 0.3 * jax.random.normal(part_keys[5], (BATCH_SIZE, 6, MODEL_WIDTH), jnp.float32) + gate_offset
    pos_common = jax.random.normal(shared_keys[0], (1, MODEL_WIDTH), jnp.float32)
    pos_frames = jax.random.normal(shared_keys[1], (NUM_FRAMES, MODEL_WIDTH), jnp.float32)
    pos_temporal = 0.4 * pos_common + 0.4 * pos_frames
    head_shape = (NUM_HEADS, HEAD_DIM, MODEL_WIDTH)
    return {
        'latents': latents,
        'text_ctx': text_ctx,
        'modulation': modulation,
        'pos_temporal': pos_temporal,
        'w_qkv_spatial': weight_draw(shared_keys[2], (3,) + head_shape, MODEL_WIDTH),
        'w_out_spatial': weight_draw(shared_keys[3], head_shape, MODEL_WIDTH),
        'w_qkv_temporal': weight_draw(shared_keys[4], (3,) + head_shape, MODEL_WIDTH),
        'w_out_temporal': weight_draw(shared_keys[5], head_shape, MODEL_WIDTH),
        'w_query_cross': weight_draw(shared_keys[6], head_shape, MODEL_WIDTH),
        'w_kv_cross': weight_draw(shared_keys[7], (2,) + head_shape, MODEL_WIDTH),
        'w_out_cross': weight_draw(shared_keys[8], head_shape, MODEL_WIDTH),
        'w_mlp_in': weight_draw(shared_keys[9], (MODEL_WIDTH, 4 * MODEL_WIDTH), MODEL_WIDTH),
        'w_mlp_out': weight_draw(shared_keys[10], (4 * MODEL_WIDTH, MODEL_WIDTH), 4 * MODEL_WIDTH),
    }


def layer_norm(acts_in):
    centered = acts_in - jnp.mean(acts_in, axis=-1, keepdims=True)
    return centered * lax.rsqrt(jnp.mean(centered * centered, axis=-1, keepdims=True) + LN_EPS)


def attend(query_heads, key_heads, value_heads):
    scores = jnp.einsum('bqhd,bkhd->bhqk', query_heads.astype(jnp.float32), key_heads.astype(jnp.float32))
    attn_probs = jax.nn.softmax(scores * (HEAD_DIM ** -0.5), axis=-1).astype(jnp.bfloat16)
    mixed_out = jnp.einsum('bhqk,bkhd->bqhd', attn_probs.astype(jnp.float32), value_heads.astype(jnp.float32))
    return mixed_out.astype(jnp.bfloat16)


def qkv_proj(acts_in, weight):
    return jnp.einsum('bnc,jhdc->jbnhd', acts_in.astype(jnp.float32), weight.astype(jnp.float32)).astype(jnp.bfloat16)


def out_proj(mixed_in, weight):
    return jnp.einsum('bnhd,hdc->bnc', mixed_in.astype(jnp.float32), weight.astype(jnp.float32))


def reference(latents, text_ctx, modulation, pos_temporal, w_qkv_spatial, w_out_spatial, w_qkv_temporal, w_out_temporal, w_query_cross, w_kv_cross, w_out_cross, w_mlp_in, w_mlp_out):
    mod_rows = jnp.moveaxis(modulation, 1, 0)[:, :, None, :]

    def spatial_frame(frame_in):
        frame_f = frame_in.astype(jnp.float32)
        normed = (layer_norm(frame_f) * (1.0 + mod_rows[1]) + mod_rows[0]).astype(jnp.bfloat16)
        qkv_all = qkv_proj(normed, w_qkv_spatial)
        mixed_out = attend(qkv_all[0], qkv_all[1], qkv_all[2])
        return (frame_f + mod_rows[2] * out_proj(mixed_out, w_out_spatial)).astype(jnp.bfloat16)

    def temporal_patch(column_in):
        column_f = column_in.astype(jnp.float32)
        shifted = (column_f + pos_temporal[None]).astype(jnp.bfloat16)
        qkv_all = qkv_proj(shifted, w_qkv_temporal)
        mixed_out = attend(qkv_all[0], qkv_all[1], qkv_all[2])
        return (column_f + mod_rows[2] * out_proj(mixed_out, w_out_temporal)).astype(jnp.bfloat16)

    ctx_kv = qkv_proj(text_ctx, w_kv_cross)

    def cross_mlp_frame(frame_in):
        frame_f = frame_in.astype(jnp.float32)
        query_heads = qkv_proj(frame_in, w_query_cross[None])[0]
        mixed_out = attend(query_heads, ctx_kv[0], ctx_kv[1])
        after_cross = (frame_f + out_proj(mixed_out, w_out_cross)).astype(jnp.bfloat16)
        cross_f = after_cross.astype(jnp.float32)
        normed = (layer_norm(cross_f) * (1.0 + mod_rows[4]) + mod_rows[3]).astype(jnp.bfloat16)
        flat_rows = normed.reshape(-1, MODEL_WIDTH)
        mlp_hidden = jax.nn.gelu(jnp.dot(flat_rows, w_mlp_in, preferred_element_type=jnp.float32), approximate=True).astype(jnp.bfloat16)
        mlp_out = jnp.dot(mlp_hidden, w_mlp_out, preferred_element_type=jnp.float32).reshape(cross_f.shape)
        return (cross_f + mod_rows[5] * mlp_out).astype(jnp.bfloat16)

    after_spatial = lax.map(spatial_frame, jnp.moveaxis(latents, 1, 0))
    after_temporal = lax.map(temporal_patch, jnp.transpose(after_spatial, (2, 1, 0, 3)))
    out_frames = lax.map(cross_mlp_frame, jnp.transpose(after_temporal, (2, 1, 0, 3)))
    return jnp.moveaxis(out_frames, 0, 1)
```

```python
import functools
import math

import jax
import jax.numpy as jnp
from jax import lax
from jax.experimental import pallas as pl
from jax.experimental.pallas import tpu as pltpu
from jax.sharding import PartitionSpec as P

LN_EPS = 1e-6
F32 = jnp.float32
BF16 = jnp.bfloat16
NT = (((1,), (1,)), ((), ()))
NN = (((1,), (0,)), ((), ()))
VMEM_LIMIT = 67_000_000


def dot_nt(lhs, rhs):
    return lax.dot_general(lhs, rhs, NT, preferred_element_type=F32)


def dot_nn(lhs, rhs):
    return lax.dot_general(lhs, rhs, NN, preferred_element_type=F32)


def normalize(rows):
    centered = rows - jnp.mean(rows, axis=-1, keepdims=True)
    return centered * lax.rsqrt(jnp.mean(centered * centered, axis=-1, keepdims=True) + LN_EPS)


def head_masks(pair, dim):
    lane = lax.broadcasted_iota(jnp.int32, (1, 256), 1)
    low = 16 * pair
    first = (lane >= low) & (lane < low + dim)
    second = (lane >= low + dim) & (lane < low + 2 * dim)
    return first.astype(BF16), second.astype(BF16)


def inverse_scale(pair, dim, inv_one, inv_two):
    edge = 16 * pair + dim
    lane = lax.broadcasted_iota(jnp.int32, (1, 128), 1)
    if edge < 128:
        return jnp.where(lane < edge, inv_one, inv_two), inv_two
    return inv_one, jnp.where(lane + 128 < edge, inv_one, inv_two)


def store_window(attn, rows, pair, pairs, mixed, scales, high):
    low = mixed[:, :128] * scales[0]
    if high is not None:
        low = low + high
    attn[rows, pl.ds(128 * pair, 128)] = low.astype(BF16)
    high = mixed[:, 128:] * scales[1]
    if pair == pairs - 1:
        attn[rows, pl.ds(128 * pairs, 128)] = high.astype(BF16)
    return high


def spatial_kernel(base_ref, x_ref, mod_ref, wqkv_hbm, wout_hbm, o_ref,
                   wqkv, wout, u, qkv, attn, ks, vs0, vs1, vs2, s0, s1, p0, p1, i0, i1, sem, *, dim):
    tokens, width = u.shape
    vs_slots, s_slots, p_slots, i_slots = (vs0, vs1, vs2), (s0, s1), (p0, p1), (i0, i1)
    first_step = pl.program_id(0) == 0
    starts = list(range(0, width, 256))

    def rows_of(part, c):
        return pl.ds(part * width + starts[c], min(256, width - starts[c]))

    early = [pltpu.make_async_copy(wqkv_hbm.at[rows_of(k, 0)], wqkv.at[rows_of(k, 0)], sem.at[k]) for k in range(3)]
    late = [pltpu.make_async_copy(wqkv_hbm.at[pl.ds(k * width + 256, width - 256)], wqkv.at[pl.ds(k * width + 256, width - 256)], sem.at[3 + k]) for k in range(3)]
    late.append(pltpu.make_async_copy(wout_hbm, wout, sem.at[6]))

    @pl.when(first_step)
    def _():
        for cp in early + late:
            cp.start()

    scale_row = 1.0 + mod_ref[0, 1:2, :]
    shift_row = mod_ref[0, 0:1, :]
    half = tokens // 2

    def modulate(low):
        for i in range(half // 48):
            rows = pl.ds(low + 48 * i, 48)
            u[rows, :] = (normalize(x_ref[0, 0, rows, :].astype(F32)) * scale_row + shift_row).astype(BF16)

    def project(c, rows):
        size = min(256, width - starts[c])
        if size == 256:
            for k in range(3):
                qkv[rows, pl.ds(k * width + starts[c], size)] = dot_nt(u[rows, :], wqkv[rows_of(k, c), :]).astype(BF16)
        else:
            out = dot_nt(u[rows, :], jnp.concatenate([wqkv[rows_of(k, c), :] for k in range(3)], 0)).astype(BF16)
            for k in range(3):
                qkv[rows, pl.ds(k * width + starts[c], size)] = out[:, k * size:(k + 1) * size]

    modulate(0)

    @pl.when(first_step)
    def _():
        for cp in early:
            cp.wait()

    project(0, pl.ds(0, half))
    modulate(half)
    project(0, pl.ds(half, half))

    @pl.when(first_step)
    def _():
        for cp in late:
            cp.wait()

    factor = math.log2(math.e) / math.sqrt(dim)
    pairs = width // (2 * dim)
    main = (tokens // 128) * 128
    lane = lax.broadcasted_iota(jnp.int32, (1, 128), 1)
    in_first = lane < (tokens - main)
    high = None

    def scores(pair):
        first, second = head_masks(pair, dim)
        k_win = qkv[:, pl.ds(width + 128 * pair, 256)]
        v_win = qkv[:, pl.ds(2 * width + 128 * pair, 256)]
        for dst, src in ((ks, k_win), (vs_slots[pair % 3], v_win)):
            one, two = src * first, src * second
            dst[0:main, :] = one[:main]
            dst[main:2 * main, :] = two[:main]
            dst[2 * main:main + tokens, :] = one[main:]
            dst[main + tokens:2 * tokens, :] = two[main:]
        s_slots[pair % 2][...] = dot_nt(qkv[:, pl.ds(128 * pair, 256)], ks[...])

    def probs(pair):
        s_ref, p_ref, i_ref = s_slots[pair % 2], p_slots[pair % 2], i_slots[pair % 2]
        for i in range(tokens // 16):
            rows = pl.ds(16 * i, 16)
            one = s_ref[rows, 0:main]
            two = s_ref[rows, main:2 * main]
            tail = s_ref[rows, 2 * main:2 * tokens]
            max_one, max_two = one[:, :128], two[:, :128]
            for c in range(128, main, 128):
                max_one = jnp.maximum(max_one, one[:, c:c + 128])
                max_two = jnp.maximum(max_two, two[:, c:c + 128])
            max_one = jnp.max(jnp.where(in_first, jnp.maximum(max_one, tail), max_one), -1, keepdims=True) * factor
            max_two = jnp.max(jnp.where(in_first, max_two, jnp.maximum(max_two, tail)), -1, keepdims=True) * factor
            one = jnp.exp2(one * factor - max_one)
            two = jnp.exp2(two * factor - max_two)
            tail = jnp.exp2(tail * factor - jnp.where(in_first, max_one, max_two))
            p_ref[rows, 0:main] = one.astype(BF16)
            p_ref[rows, main:2 * main] = two.astype(BF16)
            p_ref[rows, 2 * main:2 * tokens] = tail.astype(BF16)
            sum_one, sum_two = one[:, :128], two[:, :128]
            for c in range(128, main, 128):
                sum_one = sum_one + one[:, c:c + 128]
                sum_two = sum_two + two[:, c:c + 128]
            sum_one = jnp.sum(sum_one + jnp.where(in_first, tail, 0.0), -1, keepdims=True)
            sum_two = jnp.sum(sum_two + jnp.where(in_first, 0.0, tail), -1, keepdims=True)
            i_ref[rows, 0:128] = jnp.broadcast_to(1.0 / sum_one, (16, 128))
            i_ref[rows, 128:256] = jnp.broadcast_to(1.0 / sum_two, (16, 128))

    for step in range(pairs + 2):
        if step >= 2:
            pair = step - 2
            i_ref = i_slots[pair % 2]
            mixed = dot_nn(p_slots[pair % 2][...], vs_slots[pair % 3][...])
            scales = inverse_scale(pair, dim, i_ref[:, 0:128], i_ref[:, 128:256])
            high = store_window(attn, slice(None), pair, pairs, mixed, scales, high)
        if step < pairs:
            if step % 2 == 1 or step == 0:
                if (step + 1) // 2 + (step == 0) < len(starts):
                    project((step + 1) // 2 + (step == 0), slice(None))
            scores(step)
        if 1 <= step <= pairs:
            probs(step - 1)

    parts, rows_per = o_ref.shape[:2]
    gate = mod_ref[0, 2:3, :]
    branch = dot_nn(attn[...], wout[...])
    x_all = x_ref[0, 0].astype(F32)
    for part in range(parts):
        low = rows_per * part
        o_ref[part] = (x_all[low:low + rows_per] + gate * branch[low:low + rows_per]).astype(BF16)


def temporal_kernel(base_ref, pos_ref, mod_ref, h_hbm, wqkv_hbm, wout_hbm, o_hbm,
                    h_ref, o_ref, wqkv, wout, z, qkv, attn, s0, s1, p0, p1, i0, i1, sem, in_sem, out_sem, *, dim):
    parts, rows, width = h_ref.shape
    s_slots, p_slots, i_slots = (s0, s1), (p0, p1), (i0, i1)
    groups = rows // 16
    group_rows = 16 * parts
    span = 3
    span_rows = span * group_rows
    cuts = (0, 1280, 2560, 3 * width)
    loads = [pltpu.make_async_copy(h_hbm.at[part], h_ref.at[part], in_sem.at[part]) for part in range(parts)]
    weights = [pltpu.make_async_copy(wqkv_hbm.at[pl.ds(cuts[k], cuts[k + 1] - cuts[k])], wqkv.at[pl.ds(cuts[k], cuts[k + 1] - cuts[k])], sem.at[k]) for k in range(3)]
    weights.append(pltpu.make_async_copy(wout_hbm, wout, sem.at[3]))
    for cp in loads[:parts // 2] + weights[:1] + loads[parts // 2:] + weights[1:]:
        cp.start()
    for cp in loads:
        cp.wait()

    for part in range(parts):
        shifted = (h_ref[part].astype(F32) + pos_ref[part:part + 1, :]).astype(BF16)
        for g in range(groups):
            z[pl.ds(g * group_rows + 16 * part, 16), :] = shifted[16 * g:16 * g + 16]
    def project(c, k):
        block = pl.ds(c * span_rows, span_rows)
        qkv[block, cuts[k]:cuts[k + 1]] = dot_nt(z[block, :], wqkv[cuts[k]:cuts[k + 1], :]).astype(BF16)

    for k in range(3):
        weights[k].wait()
        if k == 2:
            weights[3].wait()
        project(0, k)

    factor = math.log2(math.e) / math.sqrt(dim)
    pairs = width // (2 * dim)
    same = (lax.rem(lax.broadcasted_iota(jnp.int32, (16, group_rows), 1), 16)
            == lax.broadcasted_iota(jnp.int32, (16, group_rows), 0))

    def block_of(g):
        return pl.ds(g * group_rows, group_rows)

    def scores(g):
        for pair in range(pairs):
            first, second = head_masks(pair, dim)
            q_win = qkv[block_of(g), pl.ds(128 * pair, 256)]
            k_win = qkv[block_of(g), pl.ds(width + 128 * pair, 256)]
            s_slots[g % 2][pair] = dot_nt(q_win, jnp.concatenate([k_win * first, k_win * second], 0))

    def probs(g):
        for pair in range(pairs):
            for i in range(group_rows // 16):
                at = pl.ds(16 * i, 16)
                for k in range(2):
                    cols = pl.ds(group_rows * k, group_rows)
                    s = jnp.where(same, s_slots[g % 2][pair, at, cols] * factor, -jnp.inf)
                    e = jnp.exp2(s - jnp.max(s, -1, keepdims=True))
                    p_slots[g % 2][pair, at, cols] = e.astype(BF16)
                    i_slots[g % 2][pair, at, cols] = jnp.broadcast_to(1.0 / jnp.sum(e, -1, keepdims=True), (16, group_rows))

    def mix(g):
        high = None
        for pair in range(pairs):
            first, second = head_masks(pair, dim)
            v_win = qkv[block_of(g), pl.ds(2 * width + 128 * pair, 256)]
            mixed = dot_nn(p_slots[g % 2][pair], jnp.concatenate([v_win * first, v_win * second], 0))
            inv = i_slots[g % 2][pair]
            scales = inverse_scale(pair, dim, inv[:, :128], inv[:, 128:])
            high = store_window(attn, block_of(g), pair, pairs, mixed, scales, high)

    videos = mod_ref.shape[0]
    per_video = rows // videos

    def finish(c):
        branch = dot_nn(attn[pl.ds(c * span_rows, span_rows), :], wout[...])
        for k in range(span):
            g = c * span + k
            index = lax.broadcasted_iota(jnp.int32, (16, 1), 0) + 16 * g
            gate = mod_ref[0, 2:3, :]
            for v in range(1, videos):
                gate = jnp.where(index >= v * per_video, mod_ref[v, 2:3, :], gate)
            for part in range(parts):
                base = k * group_rows + 16 * part
                hid = h_ref[part, pl.ds(16 * g, 16), :].astype(F32)
                o_ref[part, pl.ds(16 * g, 16), :] = (hid + gate * branch[base:base + 16]).astype(BF16)

    for step in range(groups + 2):
        if step // span + 1 < groups // span:
            project(step // span + 1, step % span)
        if step >= 2:
            mix(step - 2)
        if step < groups:
            scores(step)
        if 1 <= step <= groups:
            probs(step - 1)
        if step >= 2 and (step - 2) % span == span - 1:
            finish((step - 2) // span)

    stores = [pltpu.make_async_copy(o_ref, o_hbm, out_sem.at[0])]
    for cp in stores:
        cp.start()
    for cp in stores:
        cp.wait()


def text_kernel(t_ref, w_ref, o_ref):
    o_ref[...] = dot_nt(t_ref[...], w_ref[...]).astype(BF16)


def cross_mlp_kernel(h_ref, mod_ref, kv_ref, wq_hbm, wo_hbm, win_hbm, wdown_hbm, *refs, dim, aliased):
    refs = refs[1:] if aliased else refs
    o_ref, wq, wo, win, wdown, h, q, attn, kpad, hid, s0, s1, p0, p1, i0, i1, sem = refs
    s_slots, p_slots, i_slots = (s0, s1), (p0, p1), (i0, i1)
    tokens, width = h.shape
    parts, rows_per = h_ref.shape[:2]
    text = kv_ref.shape[1]
    first_step = pl.program_id(0) == 0
    copies = [pltpu.make_async_copy(src, dst, sem.at[i]) for i, (src, dst) in
              enumerate(((wq_hbm, wq), (wo_hbm, wo), (win_hbm, win), (wdown_hbm, wdown)))]

    @pl.when(first_step)
    def _():
        for cp in copies:
            cp.start()

    for part in range(parts):
        h[pl.ds(part * rows_per, rows_per), :] = h_ref[part].astype(F32)
    span = kpad.shape[0]
    kpad[text:, :] = jnp.zeros((span - text, 2 * width), BF16)
    kpad[:text, :] = kv_ref[0]

    @pl.when(first_step)
    def _():
        copies[0].wait()
        copies[1].wait()

    q[...] = dot_nt(h[...].astype(BF16), wq[...]).astype(BF16)

    factor = math.log2(math.e) / math.sqrt(dim)
    pairs = width // (2 * dim)
    valid = lax.broadcasted_iota(jnp.int32, (1, 128), 1) < text - (span - 128)
    high = None

    def scores(pair):
        first, second = head_masks(pair, dim)
        k_win = kpad[:, pl.ds(128 * pair, 256)]
        s_slots[pair % 2][...] = dot_nt(q[:, pl.ds(128 * pair, 256)], jnp.concatenate([k_win * first, k_win * second], 0))

    def probs(pair):
        s_ref, p_ref, i_ref = s_slots[pair % 2], p_slots[pair % 2], i_slots[pair % 2]
        for i in range(tokens // 16):
            at = pl.ds(16 * i, 16)
            for k in range(2):
                tiles = [s_ref[at, pl.ds(span * k + c, 128)] * factor for c in range(0, span, 128)]
                tiles[-1] = jnp.where(valid, tiles[-1], -jnp.inf)
                top = jnp.max(functools.reduce(jnp.maximum, tiles), -1, keepdims=True)
                tiles = [jnp.exp2(t - top) for t in tiles]
                for n, t in enumerate(tiles):
                    p_ref[at, pl.ds(span * k + 128 * n, 128)] = t.astype(BF16)
                inv = 1.0 / jnp.sum(sum(tiles[1:], tiles[0]), -1, keepdims=True)
                i_ref[at, pl.ds(128 * k, 128)] = jnp.broadcast_to(inv, (16, 128))

    for step in range(pairs + 2):
        if step >= 2:
            pair = step - 2
            first, second = head_masks(pair, dim)
            i_ref = i_slots[pair % 2]
            v_win = kpad[:, pl.ds(width + 128 * pair, 256)]
            mixed = dot_nn(p_slots[pair % 2][...], jnp.concatenate([v_win * first, v_win * second], 0))
            scales = inverse_scale(pair, dim, i_ref[:, 0:128], i_ref[:, 128:256])
            high = store_window(attn, slice(None), pair, pairs, mixed, scales, high)
        if step < pairs:
            scores(step)
        if 1 <= step <= pairs:
            probs(step - 1)

    scale_row = 1.0 + mod_ref[0, 4:5, :]
    shift_row = mod_ref[0, 3:4, :]
    half = tokens // 2
    for low in (0, half):
        block = pl.ds(low, half)
        h[block, :] = (h[block, :] + dot_nn(attn[block, :], wo[...])).astype(BF16).astype(F32)
        for i in range(half // 48):
            rows = pl.ds(low + 48 * i, 48)
            q[rows, :] = (normalize(h[rows, :]) * scale_row + shift_row).astype(BF16)

    @pl.when(first_step)
    def _():
        copies[2].wait()

    inner = win.shape[1]
    chunk = inner // 2

    @pl.loop(0, 2)
    def _(c):
        cols = pl.ds(pl.multiple_of(c * chunk, 128), chunk)
        t = dot_nn(q[...], win[:, cols])
        hid[:, cols] = jax.nn.gelu(t, approximate=True).astype(BF16)

    @pl.when(first_step)
    def _():
        copies[3].wait()

    o_ref[0, 0] = (h[...] + mod_ref[0, 5:6, :] * dot_nn(hid[...], wdown[...])).astype(BF16)


def any_spec():
    return pl.BlockSpec(memory_space=pl.ANY)


def params():
    return pltpu.CompilerParams(vmem_limit_bytes=VMEM_LIMIT, dimension_semantics=("arbitrary",))


def cost(flops, moved):
    return pl.CostEstimate(flops=flops, transcendentals=0, bytes_accessed=moved)


def spatial_call(latents, modulation, wqkv, wout, base, videos, parts, dim):
    tokens, width = latents.shape[2:]
    rows_per = tokens // parts
    pads = 2 * tokens
    flops = videos * (2 * tokens * width * 4 * width + 4 * tokens * tokens * width)
    return pl.pallas_call(
        functools.partial(spatial_kernel, dim=dim),
        grid_spec=pltpu.PrefetchScalarGridSpec(
            num_scalar_prefetch=1,
            grid=(videos,),
            in_specs=[pl.BlockSpec((1, 1, tokens, width), lambda i, at: (at[0] + i, 0, 0, 0)),
                      pl.BlockSpec((1,) + modulation.shape[1:], lambda i, at: (at[0] + i, 0, 0)),
                      any_spec(), any_spec()],
            out_specs=pl.BlockSpec((parts, rows_per, width), lambda i, at: (0, i, 0)),
            scratch_shapes=[pltpu.VMEM(wqkv.shape, BF16), pltpu.VMEM(wout.shape, BF16),
                        pltpu.VMEM((tokens, width), BF16), pltpu.VMEM((tokens, 3 * width), BF16),
                        pltpu.VMEM((tokens, width), BF16), pltpu.VMEM((pads, 256), BF16)]
        + [pltpu.VMEM((pads, 256), BF16)] * 3 + [pltpu.VMEM((tokens, pads), F32)] * 2
        + [pltpu.VMEM((tokens, pads), BF16)] * 2 + [pltpu.VMEM((tokens, 256), F32)] * 2
        + [pltpu.SemaphoreType.DMA((7,))]),
        out_shape=jax.ShapeDtypeStruct((parts, videos * rows_per, width), BF16),
        compiler_params=params(),
        cost_estimate=cost(flops, 20_000_000),
        name="spatial",
    )(base, latents, modulation, wqkv, wout)


def temporal_call(pos, modulation, pieces, wqkv, wout, base, videos, dim):
    parts, rows, width = pieces.shape
    total = rows * parts
    group_rows = 16 * parts
    pairs = width // (2 * dim)
    flops = 2 * total * width * 4 * width + 4 * total * 256 * width
    return pl.pallas_call(
        functools.partial(temporal_kernel, dim=dim),
        grid_spec=pltpu.PrefetchScalarGridSpec(
            num_scalar_prefetch=1,
            grid=(1,),
            in_specs=[pl.BlockSpec(pos.shape, lambda i, at: (0, 0)),
                      pl.BlockSpec((videos,) + modulation.shape[1:], lambda i, at: (at[0] // videos, 0, 0)),
                      any_spec(), any_spec(), any_spec()],
            out_specs=any_spec(),
            scratch_shapes=[pltpu.VMEM(pieces.shape, BF16), pltpu.VMEM(pieces.shape, BF16),
                        pltpu.VMEM(wqkv.shape, BF16), pltpu.VMEM(wout.shape, BF16),
                        pltpu.VMEM((total, width), BF16), pltpu.VMEM((total, 3 * width), BF16),
                        pltpu.VMEM((total, width), BF16)]
        + [pltpu.VMEM((pairs, group_rows, 2 * group_rows), F32)] * 2
        + [pltpu.VMEM((pairs, group_rows, 2 * group_rows), BF16)] * 2
        + [pltpu.VMEM((pairs, group_rows, 2 * group_rows), F32)] * 2
        + [pltpu.SemaphoreType.DMA((4,)), pltpu.SemaphoreType.DMA((parts,)), pltpu.SemaphoreType.DMA((1,))]),
        out_shape=jax.ShapeDtypeStruct(pieces.shape, BF16),
        compiler_params=params(),
        cost_estimate=cost(flops, 20_000_000),
        name="temporal",
    )(base, pos, modulation, pieces, wqkv, wout)


def text_call(text_ctx, w_kv):
    videos, text, width = text_ctx.shape
    outer = w_kv.shape[0]
    block = 768
    rows = text_ctx.reshape(videos * text, width)
    kv = pl.pallas_call(
        text_kernel,
        grid=(outer // block,),
        in_specs=[pl.BlockSpec(rows.shape, lambda i: (0, 0)), pl.BlockSpec((block, width), lambda i: (i, 0))],
        out_specs=pl.BlockSpec((videos * text, block), lambda i: (0, i)),
        out_shape=jax.ShapeDtypeStruct((videos * text, outer), BF16),
        compiler_params=params(),
        cost_estimate=cost(2 * videos * text * width * outer, 10_000_000),
        name="text_kv",
    )(rows, w_kv)
    return kv.reshape(videos, text, outer)


def cross_mlp_call(pieces, modulation, kv, wq, wo, win, wdown, prev, base, videos, like, dim):
    parts, rows, width = pieces.shape
    text = kv.shape[1]
    inner = win.shape[1]
    rows_per = rows // videos
    tokens = rows_per * parts
    span = ((text + 127) // 128) * 128
    flops = videos * (2 * tokens * width * (2 * width + 2 * inner) + 8 * tokens * span * width)
    aliased = prev is not None
    ins = [pieces, modulation, kv, wq, wo, win, wdown] + ([prev] if aliased else [])
    in_specs = ([pl.BlockSpec((parts, rows_per, width), lambda i: (0, i, 0)),
                 pl.BlockSpec((1,) + modulation.shape[1:], lambda i: (base + i, 0, 0)),
                 pl.BlockSpec((1, text, 2 * width), lambda i: (base + i, 0, 0))]
                + [any_spec()] * (5 if aliased else 4))
    return pl.pallas_call(
        functools.partial(cross_mlp_kernel, dim=dim, aliased=aliased),
        grid=(videos,),
        in_specs=in_specs,
        out_specs=pl.BlockSpec((1, 1, tokens, width), lambda i: (base + i, 0, 0, 0)),
        out_shape=jax.ShapeDtypeStruct(like.shape, BF16),
        scratch_shapes=[pltpu.VMEM(wq.shape, BF16), pltpu.VMEM(wo.shape, BF16),
                        pltpu.VMEM(win.shape, BF16), pltpu.VMEM(wdown.shape, BF16),
                        pltpu.VMEM((tokens, width), F32), pltpu.VMEM((tokens, width), BF16),
                        pltpu.VMEM((tokens, width), BF16), pltpu.VMEM((span, 2 * width), BF16),
                        pltpu.VMEM((tokens, inner), BF16)]
        + [pltpu.VMEM((tokens, 2 * span), F32)] * 2 + [pltpu.VMEM((tokens, 2 * span), BF16)] * 2
        + [pltpu.VMEM((tokens, 256), F32)] * 2 + [pltpu.SemaphoreType.DMA((4,))],
        input_output_aliases={len(ins) - 1: 0} if aliased else {},
        compiler_params=params(),
        cost_estimate=cost(flops, 40_000_000),
        name="cross_mlp",
    )(*ins)


CHUNK = 2


def solution(mesh):
    act_spec = P('dp', 'sp', None, None)
    row_spec = P('dp', None, None)
    rep_two = P(None, None)
    rep_three = P(None, None, None)
    rep_four = P(None, None, None, None)
    in_specs = (act_spec, row_spec, row_spec, rep_two, rep_four, rep_three, rep_four, rep_three, rep_three, rep_four, rep_three, rep_two, rep_two)
    parts = mesh.shape['sp']

    def exchange(sent):
        return lax.all_to_all(sent, 'sp', 0, 0, tiled=True)

    def local_block(latents, text_ctx, modulation, pos_temporal, w_qkv_spatial, w_out_spatial, w_qkv_temporal, w_out_temporal, w_query_cross, w_kv_cross, w_out_cross, w_mlp_in, w_mlp_out):
        videos, _, tokens, width = latents.shape
        dim = w_out_spatial.shape[1]
        flat = lambda w: w.reshape(-1, width)
        chunks = range(0, videos, CHUNK)
        first = []
        for base in chunks:
            first.append(exchange(spatial_call(latents, modulation, flat(w_qkv_spatial), flat(w_out_spatial), jnp.full((1,), base, jnp.int32), CHUNK, parts, dim)))
        second = []
        for n, base in enumerate(chunks):
            back = temporal_call(pos_temporal, modulation, first[n], flat(w_qkv_temporal), flat(w_out_temporal), jnp.full((1,), base, jnp.int32), CHUNK, dim)
            if n == 0:
                _, text_in = lax.optimization_barrier((first[0], text_ctx))
                kv = text_call(text_in, flat(w_kv_cross))
                back, kv = lax.optimization_barrier((back, kv))
            second.append(exchange(back))
        y = None
        for n, base in enumerate(chunks):
            y = cross_mlp_call(second[n], modulation, kv, flat(w_query_cross), flat(w_out_cross), w_mlp_in, w_mlp_out, y, base, CHUNK, latents, dim)
        return y

    return jax.shard_map(local_block, mesh=mesh, in_specs=in_specs, out_specs=act_spec, check_vma=False)
```

```python
import functools
import math

import jax
import jax.numpy as jnp
from jax import lax
from jax.experimental import pallas as pl
from jax.experimental.pallas import tpu as pltpu
from jax.sharding import PartitionSpec as P

LN_EPS = 1e-6
F32 = jnp.float32
BF16 = jnp.bfloat16
NT = (((1,), (1,)), ((), ()))
NN = (((1,), (0,)), ((), ()))
VMEM_LIMIT = 67_000_000


def dot_nt(lhs, rhs):
    return lax.dot_general(lhs, rhs, NT, preferred_element_type=F32)


def dot_nn(lhs, rhs):
    return lax.dot_general(lhs, rhs, NN, preferred_element_type=F32)


def normalize(rows):
    centered = rows - jnp.mean(rows, axis=-1, keepdims=True)
    return centered * lax.rsqrt(jnp.mean(centered * centered, axis=-1, keepdims=True) + LN_EPS)


def head_masks(pair, dim):
    lane = lax.broadcasted_iota(jnp.int32, (1, 256), 1)
    low = 16 * pair
    first = (lane >= low) & (lane < low + dim)
    second = (lane >= low + dim) & (lane < low + 2 * dim)
    return first.astype(BF16), second.astype(BF16)


def inverse_scale(pair, dim, inv_one, inv_two):
    edge = 16 * pair + dim
    lane = lax.broadcasted_iota(jnp.int32, (1, 128), 1)
    if edge < 128:
        return jnp.where(lane < edge, inv_one, inv_two), inv_two
    return inv_one, jnp.where(lane + 128 < edge, inv_one, inv_two)


def store_window(attn, rows, pair, pairs, mixed, scales, high):
    low = mixed[:, :128] * scales[0]
    if high is not None:
        low = low + high
    attn[rows, pl.ds(128 * pair, 128)] = low.astype(BF16)
    high = mixed[:, 128:] * scales[1]
    if pair == pairs - 1:
        attn[rows, pl.ds(128 * pairs, 128)] = high.astype(BF16)
    return high


def spatial_kernel(base_ref, x_ref, mod_ref, wqkv_hbm, wout_hbm, o_ref,
                   wqkv, wout, u, qkv, attn, ks, vs0, vs1, vs2, s0, s1, p0, p1, i0, i1, sem, *, dim):
    tokens, width = u.shape
    vs_slots, s_slots, p_slots, i_slots = (vs0, vs1, vs2), (s0, s1), (p0, p1), (i0, i1)
    first_step = pl.program_id(0) == 0
    video = pl.ds(base_ref[0] + pl.program_id(0), 1)
    starts = list(range(0, width, 256))

    def rows_of(part, c):
        return pl.ds(part * width + starts[c], min(256, width - starts[c]))

    early = [pltpu.make_async_copy(wqkv_hbm.at[rows_of(k, 0)], wqkv.at[rows_of(k, 0)], sem.at[k]) for k in range(3)]
    late = [pltpu.make_async_copy(wqkv_hbm.at[pl.ds(k * width + 256, width - 256)], wqkv.at[pl.ds(k * width + 256, width - 256)], sem.at[3 + k]) for k in range(3)]
    late.append(pltpu.make_async_copy(wout_hbm, wout, sem.at[6]))

    @pl.when(first_step)
    def _():
        for cp in early + late:
            cp.start()

    scale_row = 1.0 + mod_ref[1, video, :]
    shift_row = mod_ref[0, video, :]
    half = tokens // 2

    def modulate(low):
        for i in range(half // 48):
            rows = pl.ds(low + 48 * i, 48)
            u[rows, :] = (normalize(x_ref[0, 0, rows, :].astype(F32)) * scale_row + shift_row).astype(BF16)

    def project(c, rows):
        size = min(256, width - starts[c])
        if size == 256:
            for k in range(3):
                qkv[rows, pl.ds(k * width + starts[c], size)] = dot_nt(u[rows, :], wqkv[rows_of(k, c), :]).astype(BF16)
        else:
            out = dot_nt(u[rows, :], jnp.concatenate([wqkv[rows_of(k, c), :] for k in range(3)], 0)).astype(BF16)
            for k in range(3):
                qkv[rows, pl.ds(k * width + starts[c], size)] = out[:, k * size:(k + 1) * size]

    modulate(0)

    @pl.when(first_step)
    def _():
        for cp in early:
            cp.wait()

    project(0, pl.ds(0, half))
    modulate(half)
    project(0, pl.ds(half, half))

    @pl.when(first_step)
    def _():
        for cp in late:
            cp.wait()

    factor = math.log2(math.e) / math.sqrt(dim)
    pairs = width // (2 * dim)
    main = (tokens // 128) * 128
    lane = lax.broadcasted_iota(jnp.int32, (1, 128), 1)
    in_first = lane < (tokens - main)
    high = None

    def scores(pair):
        first, second = head_masks(pair, dim)
        k_win = qkv[:, pl.ds(width + 128 * pair, 256)]
        v_win = qkv[:, pl.ds(2 * width + 128 * pair, 256)]
        for dst, src in ((ks, k_win), (vs_slots[pair % 3], v_win)):
            one, two = src * first, src * second
            dst[0:main, :] = one[:main]
            dst[main:2 * main, :] = two[:main]
            dst[2 * main:main + tokens, :] = one[main:]
            dst[main + tokens:2 * tokens, :] = two[main:]
        s_slots[pair % 2][...] = dot_nt(qkv[:, pl.ds(128 * pair, 256)], ks[...])

    def probs(pair):
        s_ref, p_ref, i_ref = s_slots[pair % 2], p_slots[pair % 2], i_slots[pair % 2]
        for i in range(tokens // 16):
            rows = pl.ds(16 * i, 16)
            one = s_ref[rows, 0:main]
            two = s_ref[rows, main:2 * main]
            tail = s_ref[rows, 2 * main:2 * tokens]
            max_one, max_two = one[:, :128], two[:, :128]
            for c in range(128, main, 128):
                max_one = jnp.maximum(max_one, one[:, c:c + 128])
                max_two = jnp.maximum(max_two, two[:, c:c + 128])
            max_one = jnp.max(jnp.where(in_first, jnp.maximum(max_one, tail), max_one), -1, keepdims=True) * factor
            max_two = jnp.max(jnp.where(in_first, max_two, jnp.maximum(max_two, tail)), -1, keepdims=True) * factor
            one = jnp.exp2(one * factor - max_one)
            two = jnp.exp2(two * factor - max_two)
            tail = jnp.exp2(tail * factor - jnp.where(in_first, max_one, max_two))
            p_ref[rows, 0:main] = one.astype(BF16)
            p_ref[rows, main:2 * main] = two.astype(BF16)
            p_ref[rows, 2 * main:2 * tokens] = tail.astype(BF16)
            sum_one, sum_two = one[:, :128], two[:, :128]
            for c in range(128, main, 128):
                sum_one = sum_one + one[:, c:c + 128]
                sum_two = sum_two + two[:, c:c + 128]
            sum_one = jnp.sum(sum_one + jnp.where(in_first, tail, 0.0), -1, keepdims=True)
            sum_two = jnp.sum(sum_two + jnp.where(in_first, 0.0, tail), -1, keepdims=True)
            i_ref[rows, 0:128] = jnp.broadcast_to(1.0 / sum_one, (16, 128))
            i_ref[rows, 128:256] = jnp.broadcast_to(1.0 / sum_two, (16, 128))

    for step in range(pairs + 2):
        if step >= 2:
            pair = step - 2
            i_ref = i_slots[pair % 2]
            mixed = dot_nn(p_slots[pair % 2][...], vs_slots[pair % 3][...])
            scales = inverse_scale(pair, dim, i_ref[:, 0:128], i_ref[:, 128:256])
            high = store_window(attn, slice(None), pair, pairs, mixed, scales, high)
        if step < pairs:
            if step % 2 == 1 or step == 0:
                if (step + 1) // 2 + (step == 0) < len(starts):
                    project((step + 1) // 2 + (step == 0), slice(None))
            scores(step)
        if 1 <= step <= pairs:
            probs(step - 1)

    parts, rows_per = o_ref.shape[:2]
    gate = mod_ref[2, video, :]
    branch = dot_nn(attn[...], wout[...])
    x_all = x_ref[0, 0].astype(F32)
    for part in range(parts):
        low = rows_per * part
        o_ref[part] = (x_all[low:low + rows_per] + gate * branch[low:low + rows_per]).astype(BF16)


def temporal_kernel(base_ref, pos_ref, mod_ref, h_hbm, wqkv_hbm, wout_hbm, o_hbm,
                    h_ref, o_ref, wqkv, wout, z, qkv, attn, s0, s1, p0, p1, i0, i1, sem, in_sem, out_sem, *, dim, videos):
    parts, rows, width = h_ref.shape
    s_slots, p_slots, i_slots = (s0, s1), (p0, p1), (i0, i1)
    groups = rows // 16
    group_rows = 16 * parts
    span = 3
    span_rows = span * group_rows
    cuts = (0, 1280, 2560, 3 * width)
    piece = 16 * span

    def rows_copy(src, dst, sems, c):
        at = pl.ds(c * piece, piece)
        return pltpu.make_async_copy(src.at[:, at], dst.at[:, at], sems.at[c])

    loads = [rows_copy(h_hbm, h_ref, in_sem, c) for c in range(groups // span)]
    stores = [rows_copy(o_ref, o_hbm, out_sem, c) for c in range(groups // span)]
    weights = [pltpu.make_async_copy(wqkv_hbm.at[pl.ds(cuts[k], cuts[k + 1] - cuts[k])], wqkv.at[pl.ds(cuts[k], cuts[k + 1] - cuts[k])], sem.at[k]) for k in range(3)]
    weights.append(pltpu.make_async_copy(wout_hbm, wout, sem.at[3]))
    for cp in loads[:1] + weights[:3] + loads[1:] + weights[3:]:
        cp.start()

    def shift(c):
        at = pl.ds(c * piece, piece)
        for part in range(parts):
            shifted = (h_ref[part, at, :].astype(F32) + pos_ref[part:part + 1, :]).astype(BF16)
            for k in range(span):
                z[pl.ds((c * span + k) * group_rows + 16 * part, 16), :] = shifted[16 * k:16 * k + 16]

    loads[0].wait()
    shift(0)

    def project(c, k):
        block = pl.ds(c * span_rows, span_rows)
        qkv[block, cuts[k]:cuts[k + 1]] = dot_nt(z[block, :], wqkv[cuts[k]:cuts[k + 1], :]).astype(BF16)

    for k in range(3):
        weights[k].wait()
        if k == 2:
            for cp in loads[1:] + weights[3:]:
                cp.wait()
        project(0, k)
    for c in range(1, groups // span):
        shift(c)

    factor = math.log2(math.e) / math.sqrt(dim)
    pairs = width // (2 * dim)
    same = (lax.rem(lax.broadcasted_iota(jnp.int32, (16, group_rows), 1), 16)
            == lax.broadcasted_iota(jnp.int32, (16, group_rows), 0))

    def block_of(g):
        return pl.ds(g * group_rows, group_rows)

    def scores(g):
        for pair in range(pairs):
            first, second = head_masks(pair, dim)
            q_win = qkv[block_of(g), pl.ds(128 * pair, 256)]
            k_win = qkv[block_of(g), pl.ds(width + 128 * pair, 256)]
            s_slots[g % 2][pair] = dot_nt(q_win, jnp.concatenate([k_win * first, k_win * second], 0))

    def probs(g):
        for pair in range(pairs):
            for i in range(group_rows // 16):
                at = pl.ds(16 * i, 16)
                for k in range(2):
                    cols = pl.ds(group_rows * k, group_rows)
                    s = jnp.where(same, s_slots[g % 2][pair, at, cols] * factor, -jnp.inf)
                    e = jnp.exp2(s - jnp.max(s, -1, keepdims=True))
                    p_slots[g % 2][pair, at, cols] = e.astype(BF16)
                    i_slots[g % 2][pair, at, cols] = jnp.broadcast_to(1.0 / jnp.sum(e, -1, keepdims=True), (16, group_rows))

    def mix(g):
        high = None
        for pair in range(pairs):
            first, second = head_masks(pair, dim)
            v_win = qkv[block_of(g), pl.ds(2 * width + 128 * pair, 256)]
            mixed = dot_nn(p_slots[g % 2][pair], jnp.concatenate([v_win * first, v_win * second], 0))
            inv = i_slots[g % 2][pair]
            scales = inverse_scale(pair, dim, inv[:, :128], inv[:, 128:])
            high = store_window(attn, block_of(g), pair, pairs, mixed, scales, high)

    per_video = rows // videos

    def finish(c):
        branch = dot_nn(attn[pl.ds(c * span_rows, span_rows), :], wout[...])
        for k in range(span):
            g = c * span + k
            index = lax.broadcasted_iota(jnp.int32, (16, 1), 0) + 16 * g
            gate = mod_ref[2, pl.ds(base_ref[0], 1), :]
            for v in range(1, videos):
                gate = jnp.where(index >= v * per_video, mod_ref[2, pl.ds(base_ref[0] + v, 1), :], gate)
            for part in range(parts):
                base = k * group_rows + 16 * part
                hid = h_ref[part, pl.ds(16 * g, 16), :].astype(F32)
                o_ref[part, pl.ds(16 * g, 16), :] = (hid + gate * branch[base:base + 16]).astype(BF16)

    for step in range(groups + 2):
        if step // span + 1 < groups // span:
            project(step // span + 1, step % span)
        if step >= 2:
            mix(step - 2)
        if step < groups:
            scores(step)
        if 1 <= step <= groups:
            probs(step - 1)
        if step >= 2 and (step - 2) % span == span - 1:
            finish((step - 2) // span)
            stores[(step - 2) // span].start()

    for cp in stores:
        cp.wait()


def text_kernel(base_ref, t_ref, w_ref, o_ref):
    o_ref[...] = dot_nt(t_ref[...], w_ref[...]).astype(BF16)


def cross_mlp_kernel(h_ref, mod_ref, kv_ref, wq_hbm, wo_hbm, win_hbm, wdown_hbm, *refs, dim, aliased, base):
    refs = refs[1:] if aliased else refs
    o_ref, wq, wo, win, wdown, h, q, attn, kpad, hid, s0, s1, p0, p1, i0, i1, sem = refs
    s_slots, p_slots, i_slots = (s0, s1), (p0, p1), (i0, i1)
    tokens, width = h.shape
    parts, rows_per = h_ref.shape[:2]
    text = kv_ref.shape[1]
    first_step = pl.program_id(0) == 0
    video = pl.ds(base + pl.program_id(0), 1)
    copies = [pltpu.make_async_copy(src, dst, sem.at[i]) for i, (src, dst) in
              enumerate(((wq_hbm, wq), (wo_hbm, wo), (win_hbm, win), (wdown_hbm, wdown)))]

    @pl.when(first_step)
    def _():
        for cp in copies:
            cp.start()

    for part in range(parts):
        h[pl.ds(part * rows_per, rows_per), :] = h_ref[part].astype(F32)
    span = kpad.shape[0]
    kpad[text:, :] = jnp.zeros((span - text, 2 * width), BF16)
    kpad[:text, :] = kv_ref[0]

    @pl.when(first_step)
    def _():
        copies[0].wait()
        copies[1].wait()

    q[...] = dot_nt(h[...].astype(BF16), wq[...]).astype(BF16)

    factor = math.log2(math.e) / math.sqrt(dim)
    pairs = width // (2 * dim)
    valid = lax.broadcasted_iota(jnp.int32, (1, 128), 1) < text - (span - 128)
    high = None

    def scores(pair):
        first, second = head_masks(pair, dim)
        k_win = kpad[:, pl.ds(128 * pair, 256)]
        s_slots[pair % 2][...] = dot_nt(q[:, pl.ds(128 * pair, 256)], jnp.concatenate([k_win * first, k_win * second], 0))

    def probs(pair):
        s_ref, p_ref, i_ref = s_slots[pair % 2], p_slots[pair % 2], i_slots[pair % 2]
        for i in range(tokens // 16):
            at = pl.ds(16 * i, 16)
            for k in range(2):
                tiles = [s_ref[at, pl.ds(span * k + c, 128)] * factor for c in range(0, span, 128)]
                tiles[-1] = jnp.where(valid, tiles[-1], -jnp.inf)
                top = jnp.max(functools.reduce(jnp.maximum, tiles), -1, keepdims=True)
                tiles = [jnp.exp2(t - top) for t in tiles]
                for n, t in enumerate(tiles):
                    p_ref[at, pl.ds(span * k + 128 * n, 128)] = t.astype(BF16)
                inv = 1.0 / jnp.sum(sum(tiles[1:], tiles[0]), -1, keepdims=True)
                i_ref[at, pl.ds(128 * k, 128)] = jnp.broadcast_to(inv, (16, 128))

    for step in range(pairs + 2):
        if step >= 2:
            pair = step - 2
            first, second = head_masks(pair, dim)
            i_ref = i_slots[pair % 2]
            v_win = kpad[:, pl.ds(width + 128 * pair, 256)]
            mixed = dot_nn(p_slots[pair % 2][...], jnp.concatenate([v_win * first, v_win * second], 0))
            scales = inverse_scale(pair, dim, i_ref[:, 0:128], i_ref[:, 128:256])
            high = store_window(attn, slice(None), pair, pairs, mixed, scales, high)
        if step < pairs:
            scores(step)
        if 1 <= step <= pairs:
            probs(step - 1)

    scale_row = 1.0 + mod_ref[4, video, :]
    shift_row = mod_ref[3, video, :]
    half = tokens // 2
    for low in (0, half):
        block = pl.ds(low, half)
        h[block, :] = (h[block, :] + dot_nn(attn[block, :], wo[...])).astype(BF16).astype(F32)
        for i in range(half // 48):
            rows = pl.ds(low + 48 * i, 48)
            q[rows, :] = (normalize(h[rows, :]) * scale_row + shift_row).astype(BF16)

    @pl.when(first_step)
    def _():
        copies[2].wait()

    inner = win.shape[1]
    chunk = inner // 2

    @pl.loop(0, 2)
    def _(c):
        cols = pl.ds(pl.multiple_of(c * chunk, 128), chunk)
        t = dot_nn(q[...], win[:, cols])
        hid[:, cols] = jax.nn.gelu(t, approximate=True).astype(BF16)

    @pl.when(first_step)
    def _():
        copies[3].wait()

    o_ref[0, 0] = (h[...] + mod_ref[5, video, :] * dot_nn(hid[...], wdown[...])).astype(BF16)


def any_spec():
    return pl.BlockSpec(memory_space=pl.ANY)


def params():
    return pltpu.CompilerParams(vmem_limit_bytes=VMEM_LIMIT, dimension_semantics=("arbitrary",))


def cost(flops, moved):
    return pl.CostEstimate(flops=flops, transcendentals=0, bytes_accessed=moved)


def spatial_call(latents, modulation, wqkv, wout, base, videos, parts, dim):
    tokens, width = latents.shape[2:]
    rows_per = tokens // parts
    pads = 2 * tokens
    flops = videos * (2 * tokens * width * 4 * width + 4 * tokens * tokens * width)
    return pl.pallas_call(
        functools.partial(spatial_kernel, dim=dim),
        grid_spec=pltpu.PrefetchScalarGridSpec(
            num_scalar_prefetch=1,
            grid=(videos,),
            in_specs=[pl.BlockSpec((1, 1, tokens, width), lambda i, at: (at[0] + i, 0, 0, 0)),
                      pl.BlockSpec(modulation.shape, lambda i, at: (0, 0, 0)),
                      any_spec(), any_spec()],
            out_specs=pl.BlockSpec((parts, rows_per, width), lambda i, at: (0, i, 0)),
            scratch_shapes=[pltpu.VMEM(wqkv.shape, BF16), pltpu.VMEM(wout.shape, BF16),
                        pltpu.VMEM((tokens, width), BF16), pltpu.VMEM((tokens, 3 * width), BF16),
                        pltpu.VMEM((tokens, width), BF16), pltpu.VMEM((pads, 256), BF16)]
        + [pltpu.VMEM((pads, 256), BF16)] * 3 + [pltpu.VMEM((tokens, pads), F32)] * 2
        + [pltpu.VMEM((tokens, pads), BF16)] * 2 + [pltpu.VMEM((tokens, 256), F32)] * 2
        + [pltpu.SemaphoreType.DMA((7,))]),
        out_shape=jax.ShapeDtypeStruct((parts, videos * rows_per, width), BF16),
        compiler_params=params(),
        cost_estimate=cost(flops, 20_000_000),
        name="spatial",
    )(base, latents, modulation, wqkv, wout)


def temporal_call(pos, modulation, pieces, wqkv, wout, base, videos, dim):
    parts, rows, width = pieces.shape
    total = rows * parts
    group_rows = 16 * parts
    pairs = width // (2 * dim)
    flops = 2 * total * width * 4 * width + 4 * total * 256 * width
    return pl.pallas_call(
        functools.partial(temporal_kernel, dim=dim, videos=videos),
        grid_spec=pltpu.PrefetchScalarGridSpec(
            num_scalar_prefetch=1,
            grid=(1,),
            in_specs=[pl.BlockSpec(pos.shape, lambda i, at: (0, 0)),
                      pl.BlockSpec(modulation.shape, lambda i, at: (0, 0, 0)),
                      any_spec(), any_spec(), any_spec()],
            out_specs=any_spec(),
            scratch_shapes=[pltpu.VMEM(pieces.shape, BF16), pltpu.VMEM(pieces.shape, BF16),
                        pltpu.VMEM(wqkv.shape, BF16), pltpu.VMEM(wout.shape, BF16),
                        pltpu.VMEM((total, width), BF16), pltpu.VMEM((total, 3 * width), BF16),
                        pltpu.VMEM((total, width), BF16)]
        + [pltpu.VMEM((pairs, group_rows, 2 * group_rows), F32)] * 2
        + [pltpu.VMEM((pairs, group_rows, 2 * group_rows), BF16)] * 2
        + [pltpu.VMEM((pairs, group_rows, 2 * group_rows), F32)] * 2
        + [pltpu.SemaphoreType.DMA((4,)), pltpu.SemaphoreType.DMA((3,)), pltpu.SemaphoreType.DMA((3,))]),
        out_shape=jax.ShapeDtypeStruct(pieces.shape, BF16),
        compiler_params=params(),
        cost_estimate=cost(flops, 20_000_000),
        name="temporal",
    )(base, pos, modulation, pieces, wqkv, wout)


def text_call(text_ctx, w_kv, base, chunk):
    videos, text, width = text_ctx.shape
    outer = w_kv.shape[0]
    block = 768
    size = chunk * text
    kv = pl.pallas_call(
        text_kernel,
        grid_spec=pltpu.PrefetchScalarGridSpec(
            num_scalar_prefetch=1,
            grid=(outer // block,),
            in_specs=[pl.BlockSpec((size, width), lambda i, at: (at[0] // chunk, 0)),
                      pl.BlockSpec((block, width), lambda i, at: (i, 0))],
            out_specs=pl.BlockSpec((size, block), lambda i, at: (0, i))),
        out_shape=jax.ShapeDtypeStruct((size, outer), BF16),
        compiler_params=params(),
        cost_estimate=cost(2 * size * width * outer, 10_000_000),
        name="text_kv",
    )(base, text_ctx.reshape(videos * text, width), w_kv)
    return kv.reshape(chunk, text, outer)


def cross_mlp_call(pieces, modulation, kv, wq, wo, win, wdown, prev, base, videos, like, dim):
    parts, rows, width = pieces.shape
    text = kv.shape[1]
    inner = win.shape[1]
    rows_per = rows // videos
    tokens = rows_per * parts
    span = ((text + 127) // 128) * 128
    flops = videos * (2 * tokens * width * (2 * width + 2 * inner) + 8 * tokens * span * width)
    aliased = prev is not None
    ins = [pieces, modulation, kv, wq, wo, win, wdown] + ([prev] if aliased else [])
    in_specs = ([pl.BlockSpec((parts, rows_per, width), lambda i: (0, i, 0)),
                 pl.BlockSpec(modulation.shape, lambda i: (0, 0, 0)),
                 pl.BlockSpec((1, text, 2 * width), lambda i: (i, 0, 0))]
                + [any_spec()] * (5 if aliased else 4))
    return pl.pallas_call(
        functools.partial(cross_mlp_kernel, dim=dim, aliased=aliased, base=base),
        grid=(videos,),
        in_specs=in_specs,
        out_specs=pl.BlockSpec((1, 1, tokens, width), lambda i: (base + i, 0, 0, 0)),
        out_shape=jax.ShapeDtypeStruct(like.shape, BF16),
        scratch_shapes=[pltpu.VMEM(wq.shape, BF16), pltpu.VMEM(wo.shape, BF16),
                        pltpu.VMEM(win.shape, BF16), pltpu.VMEM(wdown.shape, BF16),
                        pltpu.VMEM((tokens, width), F32), pltpu.VMEM((tokens, width), BF16),
                        pltpu.VMEM((tokens, width), BF16), pltpu.VMEM((span, 2 * width), BF16),
                        pltpu.VMEM((tokens, inner), BF16)]
        + [pltpu.VMEM((tokens, 2 * span), F32)] * 2 + [pltpu.VMEM((tokens, 2 * span), BF16)] * 2
        + [pltpu.VMEM((tokens, 256), F32)] * 2 + [pltpu.SemaphoreType.DMA((4,))],
        input_output_aliases={len(ins) - 1: 0} if aliased else {},
        compiler_params=params(),
        cost_estimate=cost(flops, 40_000_000),
        name="cross_mlp",
    )(*ins)


CHUNK = 2


def solution(mesh):
    act_spec = P('dp', 'sp', None, None)
    row_spec = P('dp', None, None)
    rep_two = P(None, None)
    rep_three = P(None, None, None)
    rep_four = P(None, None, None, None)
    in_specs = (act_spec, row_spec, row_spec, rep_two, rep_four, rep_three, rep_four, rep_three, rep_three, rep_four, rep_three, rep_two, rep_two)
    parts = mesh.shape['sp']

    def exchange(sent):
        return lax.all_to_all(sent, 'sp', 0, 0, tiled=True)

    def local_block(latents, text_ctx, modulation, pos_temporal, w_qkv_spatial, w_out_spatial, w_qkv_temporal, w_out_temporal, w_query_cross, w_kv_cross, w_out_cross, w_mlp_in, w_mlp_out):
        videos, _, tokens, width = latents.shape
        dim = w_out_spatial.shape[1]
        flat = lambda w: w.reshape(-1, width)
        modulation = jnp.swapaxes(modulation, 0, 1)
        chunks = range(0, videos, CHUNK)
        first = []
        for base in chunks:
            first.append(exchange(spatial_call(latents, modulation, flat(w_qkv_spatial), flat(w_out_spatial), jnp.full((1,), base, jnp.int32), CHUNK, parts, dim)))
        second, kv, backs = [], [], []
        for n, base in enumerate(chunks):
            at = jnp.full((1,), base, jnp.int32)
            back = temporal_call(pos_temporal, modulation, first[n], flat(w_qkv_temporal), flat(w_out_temporal), at, CHUNK, dim)
            _, text_in = lax.optimization_barrier((backs[-1] if backs else first[0], text_ctx))
            back, kv_n = lax.optimization_barrier((back, text_call(text_in, flat(w_kv_cross), at, CHUNK)))
            kv.append(kv_n)
            backs.append(back)
            second.append(exchange(back))
        y = None
        for n, base in enumerate(chunks):
            y = cross_mlp_call(second[n], modulation, kv[n], flat(w_query_cross), flat(w_out_cross), w_mlp_in, w_mlp_out, y, base, CHUNK, latents, dim)
        return y

    return jax.shard_map(local_block, mesh=mesh, in_specs=in_specs, out_specs=act_spec, check_vma=False)
```

```python
import functools
import math

import jax
import jax.numpy as jnp
from jax import lax
from jax.experimental import pallas as pl
from jax.experimental.pallas import tpu as pltpu
from jax.sharding import PartitionSpec as P

LN_EPS = 1e-6
F32 = jnp.float32
BF16 = jnp.bfloat16
NT = (((1,), (1,)), ((), ()))
NN = (((1,), (0,)), ((), ()))
VMEM_LIMIT = 67_000_000


def dot_nt(lhs, rhs):
    return lax.dot_general(lhs, rhs, NT, preferred_element_type=F32)


def dot_nn(lhs, rhs):
    return lax.dot_general(lhs, rhs, NN, preferred_element_type=F32)


def normalize(rows):
    centered = rows - jnp.mean(rows, axis=-1, keepdims=True)
    return centered * lax.rsqrt(jnp.mean(centered * centered, axis=-1, keepdims=True) + LN_EPS)


def head_masks(pair, dim):
    lane = lax.broadcasted_iota(jnp.int32, (1, 256), 1)
    low = 16 * pair
    first = (lane >= low) & (lane < low + dim)
    second = (lane >= low + dim) & (lane < low + 2 * dim)
    return first.astype(BF16), second.astype(BF16)


def inverse_scale(pair, dim, inv_one, inv_two):
    edge = 16 * pair + dim
    lane = lax.broadcasted_iota(jnp.int32, (1, 128), 1)
    if edge < 128:
        return jnp.where(lane < edge, inv_one, inv_two), inv_two
    return inv_one, jnp.where(lane + 128 < edge, inv_one, inv_two)


def store_window(attn, rows, pair, pairs, mixed, scales, high):
    low = mixed[:, :128] * scales[0]
    if high is not None:
        low = low + high
    attn[rows, pl.ds(128 * pair, 128)] = low.astype(BF16)
    high = mixed[:, 128:] * scales[1]
    if pair == pairs - 1:
        attn[rows, pl.ds(128 * pairs, 128)] = high.astype(BF16)
    return high


def spatial_kernel(base_ref, x_ref, mod_ref, wqkv_hbm, wout_hbm, o_ref,
                   wqkv, wout, u, qkv, attn, ks, vs0, vs1, vs2, s0, s1, p0, p1, i0, i1, sem, *, dim):
    tokens, width = u.shape
    vs_slots, s_slots, p_slots, i_slots = (vs0, vs1, vs2), (s0, s1), (p0, p1), (i0, i1)
    first_step = pl.program_id(0) == 0
    video = pl.ds(base_ref[0] + pl.program_id(0), 1)
    starts = list(range(0, width, 256))

    def rows_of(part, c):
        return pl.ds(part * width + starts[c], min(256, width - starts[c]))

    early = [pltpu.make_async_copy(wqkv_hbm.at[rows_of(k, 0)], wqkv.at[rows_of(k, 0)], sem.at[k]) for k in range(3)]
    late = [pltpu.make_async_copy(wqkv_hbm.at[pl.ds(k * width + 256, width - 256)], wqkv.at[pl.ds(k * width + 256, width - 256)], sem.at[3 + k]) for k in range(3)]
    late.append(pltpu.make_async_copy(wout_hbm, wout, sem.at[6]))

    @pl.when(first_step)
    def _():
        for cp in early:
            cp.start()

    scale_row = 1.0 + mod_ref[1, video, :]
    shift_row = mod_ref[0, video, :]
    half = tokens // 2

    def modulate(low):
        for i in range(half // 48):
            rows = pl.ds(low + 48 * i, 48)
            u[rows, :] = (normalize(x_ref[0, 0, rows, :].astype(F32)) * scale_row + shift_row).astype(BF16)

    def project(c, rows):
        size = min(256, width - starts[c])
        if size == 256:
            for k in range(3):
                qkv[rows, pl.ds(k * width + starts[c], size)] = dot_nt(u[rows, :], wqkv[rows_of(k, c), :]).astype(BF16)
        else:
            out = dot_nt(u[rows, :], jnp.concatenate([wqkv[rows_of(k, c), :] for k in range(3)], 0)).astype(BF16)
            for k in range(3):
                qkv[rows, pl.ds(k * width + starts[c], size)] = out[:, k * size:(k + 1) * size]

    modulate(0)

    @pl.when(first_step)
    def _():
        for cp in early:
            cp.wait()
        for cp in late:
            cp.start()

    project(0, pl.ds(0, half))
    modulate(half)
    project(0, pl.ds(half, half))

    @pl.when(first_step)
    def _():
        for cp in late:
            cp.wait()

    factor = math.log2(math.e) / math.sqrt(dim)
    pairs = width // (2 * dim)
    main = (tokens // 128) * 128
    lane = lax.broadcasted_iota(jnp.int32, (1, 128), 1)
    in_first = lane < (tokens - main)
    high = None

    def scores(pair):
        first, second = head_masks(pair, dim)
        k_win = qkv[:, pl.ds(width + 128 * pair, 256)]
        v_win = qkv[:, pl.ds(2 * width + 128 * pair, 256)]
        for dst, src in ((ks, k_win), (vs_slots[pair % 3], v_win)):
            one, two = src * first, src * second
            dst[0:main, :] = one[:main]
            dst[main:2 * main, :] = two[:main]
            dst[2 * main:main + tokens, :] = one[main:]
            dst[main + tokens:2 * tokens, :] = two[main:]
        s_slots[pair % 2][...] = dot_nt(qkv[:, pl.ds(128 * pair, 256)], ks[...])

    def probs(pair):
        s_ref, p_ref, i_ref = s_slots[pair % 2], p_slots[pair % 2], i_slots[pair % 2]
        for i in range(tokens // 16):
            rows = pl.ds(16 * i, 16)
            one = s_ref[rows, 0:main]
            two = s_ref[rows, main:2 * main]
            tail = s_ref[rows, 2 * main:2 * tokens]
            max_one, max_two = one[:, :128], two[:, :128]
            for c in range(128, main, 128):
                max_one = jnp.maximum(max_one, one[:, c:c + 128])
                max_two = jnp.maximum(max_two, two[:, c:c + 128])
            max_one = jnp.max(jnp.where(in_first, jnp.maximum(max_one, tail), max_one), -1, keepdims=True) * factor
            max_two = jnp.max(jnp.where(in_first, max_two, jnp.maximum(max_two, tail)), -1, keepdims=True) * factor
            one = jnp.exp2(one * factor - max_one)
            two = jnp.exp2(two * factor - max_two)
            tail = jnp.exp2(tail * factor - jnp.where(in_first, max_one, max_two))
            p_ref[rows, 0:main] = one.astype(BF16)
            p_ref[rows, main:2 * main] = two.astype(BF16)
            p_ref[rows, 2 * main:2 * tokens] = tail.astype(BF16)
            sum_one, sum_two = one[:, :128], two[:, :128]
            for c in range(128, main, 128):
                sum_one = sum_one + one[:, c:c + 128]
                sum_two = sum_two + two[:, c:c + 128]
            sum_one = jnp.sum(sum_one + jnp.where(in_first, tail, 0.0), -1, keepdims=True)
            sum_two = jnp.sum(sum_two + jnp.where(in_first, 0.0, tail), -1, keepdims=True)
            i_ref[rows, 0:128] = jnp.broadcast_to(1.0 / sum_one, (16, 128))
            i_ref[rows, 128:256] = jnp.broadcast_to(1.0 / sum_two, (16, 128))

    for step in range(pairs + 2):
        if step >= 2:
            pair = step - 2
            i_ref = i_slots[pair % 2]
            mixed = dot_nn(p_slots[pair % 2][...], vs_slots[pair % 3][...])
            scales = inverse_scale(pair, dim, i_ref[:, 0:128], i_ref[:, 128:256])
            high = store_window(attn, slice(None), pair, pairs, mixed, scales, high)
        if step < pairs:
            if step % 2 == 1 or step == 0:
                if (step + 1) // 2 + (step == 0) < len(starts):
                    project((step + 1) // 2 + (step == 0), slice(None))
            scores(step)
        if 1 <= step <= pairs:
            probs(step - 1)

    parts, rows_per = o_ref.shape[:2]
    gate = mod_ref[2, video, :]
    branch = dot_nn(attn[...], wout[...])
    x_all = x_ref[0, 0].astype(F32)
    for part in range(parts):
        low = rows_per * part
        o_ref[part] = (x_all[low:low + rows_per] + gate * branch[low:low + rows_per]).astype(BF16)


def temporal_kernel(base_ref, pos_ref, mod_ref, h_hbm, wqkv_hbm, wout_hbm, o_hbm,
                    h_ref, o_ref, wqkv, wout, z, qkv, attn, s0, s1, p0, p1, i0, i1, sem, in_sem, out_sem, *, dim, videos):
    parts, rows, width = h_ref.shape
    s_slots, p_slots, i_slots = (s0, s1), (p0, p1), (i0, i1)
    groups = rows // 16
    group_rows = 16 * parts
    span = 3
    span_rows = span * group_rows
    cuts = (0, 1280, 2560, 3 * width)
    piece = 16 * span

    def rows_copy(src, dst, sems, c):
        at = pl.ds(c * piece, piece)
        return pltpu.make_async_copy(src.at[:, at], dst.at[:, at], sems.at[c])

    loads = [rows_copy(h_hbm, h_ref, in_sem, c) for c in range(groups // span)]
    stores = [rows_copy(o_ref, o_hbm, out_sem, c) for c in range(groups // span)]
    weights = [pltpu.make_async_copy(wqkv_hbm.at[pl.ds(cuts[k], cuts[k + 1] - cuts[k])], wqkv.at[pl.ds(cuts[k], cuts[k + 1] - cuts[k])], sem.at[k]) for k in range(3)]
    weights.append(pltpu.make_async_copy(wout_hbm, wout, sem.at[3]))
    for cp in loads[:1] + weights[:3] + loads[1:] + weights[3:]:
        cp.start()

    def shift(c):
        at = pl.ds(c * piece, piece)
        for part in range(parts):
            shifted = (h_ref[part, at, :].astype(F32) + pos_ref[part:part + 1, :]).astype(BF16)
            for k in range(span):
                z[pl.ds((c * span + k) * group_rows + 16 * part, 16), :] = shifted[16 * k:16 * k + 16]

    loads[0].wait()
    shift(0)

    def project(c, k):
        block = pl.ds(c * span_rows, span_rows)
        qkv[block, cuts[k]:cuts[k + 1]] = dot_nt(z[block, :], wqkv[cuts[k]:cuts[k + 1], :]).astype(BF16)

    for k in range(3):
        weights[k].wait()
        if k == 2:
            for cp in loads[1:] + weights[3:]:
                cp.wait()
        project(0, k)
    for c in range(1, groups // span):
        shift(c)

    factor = math.log2(math.e) / math.sqrt(dim)
    pairs = width // (2 * dim)
    same = (lax.rem(lax.broadcasted_iota(jnp.int32, (16, group_rows), 1), 16)
            == lax.broadcasted_iota(jnp.int32, (16, group_rows), 0))

    def block_of(g):
        return pl.ds(g * group_rows, group_rows)

    def scores(g):
        for pair in range(pairs):
            first, second = head_masks(pair, dim)
            q_win = qkv[block_of(g), pl.ds(128 * pair, 256)]
            k_win = qkv[block_of(g), pl.ds(width + 128 * pair, 256)]
            s_slots[g % 2][pair] = dot_nt(q_win, jnp.concatenate([k_win * first, k_win * second], 0))

    def probs(g):
        for pair in range(pairs):
            for i in range(group_rows // 16):
                at = pl.ds(16 * i, 16)
                for k in range(2):
                    cols = pl.ds(group_rows * k, group_rows)
                    s = jnp.where(same, s_slots[g % 2][pair, at, cols] * factor, -jnp.inf)
                    e = jnp.exp2(s - jnp.max(s, -1, keepdims=True))
                    p_slots[g % 2][pair, at, cols] = e.astype(BF16)
                    i_slots[g % 2][pair, at, cols] = jnp.broadcast_to(1.0 / jnp.sum(e, -1, keepdims=True), (16, group_rows))

    def mix(g):
        high = None
        for pair in range(pairs):
            first, second = head_masks(pair, dim)
            v_win = qkv[block_of(g), pl.ds(2 * width + 128 * pair, 256)]
            mixed = dot_nn(p_slots[g % 2][pair], jnp.concatenate([v_win * first, v_win * second], 0))
            inv = i_slots[g % 2][pair]
            scales = inverse_scale(pair, dim, inv[:, :128], inv[:, 128:])
            high = store_window(attn, block_of(g), pair, pairs, mixed, scales, high)

    per_video = rows // videos

    def finish(c):
        branch = dot_nn(attn[pl.ds(c * span_rows, span_rows), :], wout[...])
        for k in range(span):
            g = c * span + k
            index = lax.broadcasted_iota(jnp.int32, (16, 1), 0) + 16 * g
            gate = mod_ref[2, pl.ds(base_ref[0], 1), :]
            for v in range(1, videos):
                gate = jnp.where(index >= v * per_video, mod_ref[2, pl.ds(base_ref[0] + v, 1), :], gate)
            for part in range(parts):
                base = k * group_rows + 16 * part
                hid = h_ref[part, pl.ds(16 * g, 16), :].astype(F32)
                o_ref[part, pl.ds(16 * g, 16), :] = (hid + gate * branch[base:base + 16]).astype(BF16)

    for step in range(groups + 2):
        if step // span + 1 < groups // span:
            project(step // span + 1, step % span)
        if step >= 2:
            mix(step - 2)
        if step < groups:
            scores(step)
        if 1 <= step <= groups:
            probs(step - 1)
        if step >= 2 and (step - 2) % span == span - 1:
            finish((step - 2) // span)
            stores[(step - 2) // span].start()

    for cp in stores:
        cp.wait()


def text_kernel(base_ref, t_ref, w_ref, o_ref):
    o_ref[...] = dot_nt(t_ref[...], w_ref[...]).astype(BF16)


def cross_mlp_kernel(h_ref, mod_ref, kv_ref, wq_hbm, wo_hbm, win_hbm, wdown_hbm, *refs, dim, aliased, base):
    refs = refs[1:] if aliased else refs
    o_ref, wq, wo, win, wdown, h, q, attn, kpad, hid, s0, s1, p0, p1, i0, i1, sem = refs
    s_slots, p_slots, i_slots = (s0, s1), (p0, p1), (i0, i1)
    tokens, width = h.shape
    parts, rows_per = h_ref.shape[:2]
    text = kv_ref.shape[1]
    first_step = pl.program_id(0) == 0
    video = pl.ds(base + pl.program_id(0), 1)
    copies = [pltpu.make_async_copy(src, dst, sem.at[i]) for i, (src, dst) in
              enumerate(((wq_hbm, wq), (wo_hbm, wo), (win_hbm, win), (wdown_hbm, wdown)))]

    @pl.when(first_step)
    def _():
        for cp in copies[:2]:
            cp.start()

    for part in range(parts):
        h[pl.ds(part * rows_per, rows_per), :] = h_ref[part].astype(F32)
    span = kpad.shape[0]
    kpad[text:, :] = jnp.zeros((span - text, 2 * width), BF16)
    kpad[:text, :] = kv_ref[0]

    @pl.when(first_step)
    def _():
        copies[0].wait()
        copies[1].wait()
        copies[2].start()
        copies[3].start()

    q[...] = dot_nt(h[...].astype(BF16), wq[...]).astype(BF16)

    factor = math.log2(math.e) / math.sqrt(dim)
    pairs = width // (2 * dim)
    valid = lax.broadcasted_iota(jnp.int32, (1, 128), 1) < text - (span - 128)
    high = None

    def scores(pair):
        first, second = head_masks(pair, dim)
        k_win = kpad[:, pl.ds(128 * pair, 256)]
        s_slots[pair % 2][...] = dot_nt(q[:, pl.ds(128 * pair, 256)], jnp.concatenate([k_win * first, k_win * second], 0))

    def probs(pair):
        s_ref, p_ref, i_ref = s_slots[pair % 2], p_slots[pair % 2], i_slots[pair % 2]
        for i in range(tokens // 16):
            at = pl.ds(16 * i, 16)
            for k in range(2):
                tiles = [s_ref[at, pl.ds(span * k + c, 128)] * factor for c in range(0, span, 128)]
                tiles[-1] = jnp.where(valid, tiles[-1], -jnp.inf)
                top = jnp.max(functools.reduce(jnp.maximum, tiles), -1, keepdims=True)
                tiles = [jnp.exp2(t - top) for t in tiles]
                for n, t in enumerate(tiles):
                    p_ref[at, pl.ds(span * k + 128 * n, 128)] = t.astype(BF16)
                inv = 1.0 / jnp.sum(sum(tiles[1:], tiles[0]), -1, keepdims=True)
                i_ref[at, pl.ds(128 * k, 128)] = jnp.broadcast_to(inv, (16, 128))

    for step in range(pairs + 2):
        if step >= 2:
            pair = step - 2
            first, second = head_masks(pair, dim)
            i_ref = i_slots[pair % 2]
            v_win = kpad[:, pl.ds(width + 128 * pair, 256)]
            mixed = dot_nn(p_slots[pair % 2][...], jnp.concatenate([v_win * first, v_win * second], 0))
            scales = inverse_scale(pair, dim, i_ref[:, 0:128], i_ref[:, 128:256])
            high = store_window(attn, slice(None), pair, pairs, mixed, scales, high)
        if step < pairs:
            scores(step)
        if 1 <= step <= pairs:
            probs(step - 1)

    scale_row = 1.0 + mod_ref[4, video, :]
    shift_row = mod_ref[3, video, :]
    half = tokens // 2
    for low in (0, half):
        block = pl.ds(low, half)
        h[block, :] = (h[block, :] + dot_nn(attn[block, :], wo[...])).astype(BF16).astype(F32)
        for i in range(half // 48):
            rows = pl.ds(low + 48 * i, 48)
            q[rows, :] = (normalize(h[rows, :]) * scale_row + shift_row).astype(BF16)

    @pl.when(first_step)
    def _():
        copies[2].wait()
        copies[3].wait()

    inner = win.shape[1]
    for low in range(0, inner, 1536):
        cols = pl.ds(low, min(1536, inner - low))
        hid[:, cols] = jax.nn.gelu(dot_nn(q[...], win[:, cols]), approximate=True).astype(BF16)

    o_ref[0, 0] = (h[...] + mod_ref[5, video, :] * dot_nn(hid[...], wdown[...])).astype(BF16)


def any_spec():
    return pl.BlockSpec(memory_space=pl.ANY)


def params():
    return pltpu.CompilerParams(vmem_limit_bytes=VMEM_LIMIT, dimension_semantics=("arbitrary",))


def cost(flops, moved):
    return pl.CostEstimate(flops=flops, transcendentals=0, bytes_accessed=moved)


def spatial_call(latents, modulation, wqkv, wout, base, videos, parts, dim):
    tokens, width = latents.shape[2:]
    rows_per = tokens // parts
    pads = 2 * tokens
    flops = videos * (2 * tokens * width * 4 * width + 4 * tokens * tokens * width)
    return pl.pallas_call(
        functools.partial(spatial_kernel, dim=dim),
        grid_spec=pltpu.PrefetchScalarGridSpec(
            num_scalar_prefetch=1,
            grid=(videos,),
            in_specs=[pl.BlockSpec((1, 1, tokens, width), lambda i, at: (at[0] + i, 0, 0, 0)),
                      pl.BlockSpec(modulation.shape, lambda i, at: (0, 0, 0)),
                      any_spec(), any_spec()],
            out_specs=pl.BlockSpec((parts, rows_per, width), lambda i, at: (0, i, 0)),
            scratch_shapes=[pltpu.VMEM(wqkv.shape, BF16), pltpu.VMEM(wout.shape, BF16),
                        pltpu.VMEM((tokens, width), BF16), pltpu.VMEM((tokens, 3 * width), BF16),
                        pltpu.VMEM((tokens, width), BF16), pltpu.VMEM((pads, 256), BF16)]
        + [pltpu.VMEM((pads, 256), BF16)] * 3 + [pltpu.VMEM((tokens, pads), F32)] * 2
        + [pltpu.VMEM((tokens, pads), BF16)] * 2 + [pltpu.VMEM((tokens, 256), F32)] * 2
        + [pltpu.SemaphoreType.DMA((7,))]),
        out_shape=jax.ShapeDtypeStruct((parts, videos * rows_per, width), BF16),
        compiler_params=params(),
        cost_estimate=cost(flops, 20_000_000),
        name="spatial",
    )(base, latents, modulation, wqkv, wout)


def temporal_call(pos, modulation, pieces, wqkv, wout, base, videos, dim):
    parts, rows, width = pieces.shape
    total = rows * parts
    group_rows = 16 * parts
    pairs = width // (2 * dim)
    flops = 2 * total * width * 4 * width + 4 * total * 256 * width
    return pl.pallas_call(
        functools.partial(temporal_kernel, dim=dim, videos=videos),
        grid_spec=pltpu.PrefetchScalarGridSpec(
            num_scalar_prefetch=1,
            grid=(1,),
            in_specs=[pl.BlockSpec(pos.shape, lambda i, at: (0, 0)),
                      pl.BlockSpec(modulation.shape, lambda i, at: (0, 0, 0)),
                      any_spec(), any_spec(), any_spec()],
            out_specs=any_spec(),
            scratch_shapes=[pltpu.VMEM(pieces.shape, BF16), pltpu.VMEM(pieces.shape, BF16),
                        pltpu.VMEM(wqkv.shape, BF16), pltpu.VMEM(wout.shape, BF16),
                        pltpu.VMEM((total, width), BF16), pltpu.VMEM((total, 3 * width), BF16),
                        pltpu.VMEM((total, width), BF16)]
        + [pltpu.VMEM((pairs, group_rows, 2 * group_rows), F32)] * 2
        + [pltpu.VMEM((pairs, group_rows, 2 * group_rows), BF16)] * 2
        + [pltpu.VMEM((pairs, group_rows, 2 * group_rows), F32)] * 2
        + [pltpu.SemaphoreType.DMA((4,)), pltpu.SemaphoreType.DMA((3,)), pltpu.SemaphoreType.DMA((3,))]),
        out_shape=jax.ShapeDtypeStruct(pieces.shape, BF16),
        compiler_params=params(),
        cost_estimate=cost(flops, 20_000_000),
        name="temporal",
    )(base, pos, modulation, pieces, wqkv, wout)


def text_call(text_ctx, w_kv, base, chunk):
    videos, text, width = text_ctx.shape
    outer = w_kv.shape[0]
    block = 768
    size = chunk * text
    kv = pl.pallas_call(
        text_kernel,
        grid_spec=pltpu.PrefetchScalarGridSpec(
            num_scalar_prefetch=1,
            grid=(outer // block,),
            in_specs=[pl.BlockSpec((size, width), lambda i, at: (at[0] // chunk, 0)),
                      pl.BlockSpec((block, width), lambda i, at: (i, 0))],
            out_specs=pl.BlockSpec((size, block), lambda i, at: (0, i))),
        out_shape=jax.ShapeDtypeStruct((size, outer), BF16),
        compiler_params=params(),
        cost_estimate=cost(2 * size * width * outer, 10_000_000),
        name="text_kv",
    )(base, text_ctx.reshape(videos * text, width), w_kv)
    return kv.reshape(chunk, text, outer)


def cross_mlp_call(pieces, modulation, kv, wq, wo, win, wdown, prev, base, videos, like, dim):
    parts, rows, width = pieces.shape
    text = kv.shape[1]
    inner = win.shape[1]
    rows_per = rows // videos
    tokens = rows_per * parts
    span = ((text + 127) // 128) * 128
    flops = videos * (2 * tokens * width * (2 * width + 2 * inner) + 8 * tokens * span * width)
    aliased = prev is not None
    ins = [pieces, modulation, kv, wq, wo, win, wdown] + ([prev] if aliased else [])
    in_specs = ([pl.BlockSpec((parts, rows_per, width), lambda i: (0, i, 0)),
                 pl.BlockSpec(modulation.shape, lambda i: (0, 0, 0)),
                 pl.BlockSpec((1, text, 2 * width), lambda i: (i, 0, 0))]
                + [any_spec()] * (5 if aliased else 4))
    return pl.pallas_call(
        functools.partial(cross_mlp_kernel, dim=dim, aliased=aliased, base=base),
        grid=(videos,),
        in_specs=in_specs,
        out_specs=pl.BlockSpec((1, 1, tokens, width), lambda i: (base + i, 0, 0, 0)),
        out_shape=jax.ShapeDtypeStruct(like.shape, BF16),
        scratch_shapes=[pltpu.VMEM(wq.shape, BF16), pltpu.VMEM(wo.shape, BF16),
                        pltpu.VMEM(win.shape, BF16), pltpu.VMEM(wdown.shape, BF16),
                        pltpu.VMEM((tokens, width), F32), pltpu.VMEM((tokens, width), BF16),
                        pltpu.VMEM((tokens, width), BF16), pltpu.VMEM((span, 2 * width), BF16),
                        pltpu.VMEM((tokens, inner), BF16)]
        + [pltpu.VMEM((tokens, 2 * span), F32)] * 2 + [pltpu.VMEM((tokens, 2 * span), BF16)] * 2
        + [pltpu.VMEM((tokens, 256), F32)] * 2 + [pltpu.SemaphoreType.DMA((4,))],
        input_output_aliases={len(ins) - 1: 0} if aliased else {},
        compiler_params=params(),
        cost_estimate=cost(flops, 40_000_000),
        name="cross_mlp",
    )(*ins)


CHUNK = 2


def solution(mesh):
    act_spec = P('dp', 'sp', None, None)
    row_spec = P('dp', None, None)
    rep_two = P(None, None)
    rep_three = P(None, None, None)
    rep_four = P(None, None, None, None)
    in_specs = (act_spec, row_spec, row_spec, rep_two, rep_four, rep_three, rep_four, rep_three, rep_three, rep_four, rep_three, rep_two, rep_two)
    parts = mesh.shape['sp']

    def exchange(sent):
        return lax.all_to_all(sent, 'sp', 0, 0, tiled=True)

    def local_block(latents, text_ctx, modulation, pos_temporal, w_qkv_spatial, w_out_spatial, w_qkv_temporal, w_out_temporal, w_query_cross, w_kv_cross, w_out_cross, w_mlp_in, w_mlp_out):
        videos, _, tokens, width = latents.shape
        dim = w_out_spatial.shape[1]
        flat = lambda w: w.reshape(-1, width)
        modulation = jnp.swapaxes(modulation, 0, 1)
        chunks = range(0, videos, CHUNK)
        first = []
        for base in chunks:
            first.append(exchange(spatial_call(latents, modulation, flat(w_qkv_spatial), flat(w_out_spatial), jnp.full((1,), base, jnp.int32), CHUNK, parts, dim)))
        second, kv, backs = [], [], []
        for n, base in enumerate(chunks):
            at = jnp.full((1,), base, jnp.int32)
            back = temporal_call(pos_temporal, modulation, first[n], flat(w_qkv_temporal), flat(w_out_temporal), at, CHUNK, dim)
            _, text_in = lax.optimization_barrier((backs[-1] if backs else first[0], text_ctx))
            back, kv_n = lax.optimization_barrier((back, text_call(text_in, flat(w_kv_cross), at, CHUNK)))
            kv.append(kv_n)
            backs.append(back)
            second.append(exchange(back))
        y = None
        for n, base in enumerate(chunks):
            y = cross_mlp_call(second[n], modulation, kv[n], flat(w_query_cross), flat(w_out_cross), w_mlp_in, w_mlp_out, y, base, CHUNK, latents, dim)
        return y

    return jax.shard_map(local_block, mesh=mesh, in_specs=in_specs, out_specs=act_spec, check_vma=False)
```

```python
import functools
import math

import jax
import jax.numpy as jnp
from jax import lax
from jax.experimental import pallas as pl
from jax.experimental.pallas import tpu as pltpu
from jax.sharding import PartitionSpec as P

LN_EPS = 1e-6
F32 = jnp.float32
BF16 = jnp.bfloat16
NT = (((1,), (1,)), ((), ()))
NN = (((1,), (0,)), ((), ()))
VMEM_LIMIT = 67_000_000


def dot_nt(lhs, rhs):
    return lax.dot_general(lhs, rhs, NT, preferred_element_type=F32)


def dot_nn(lhs, rhs):
    return lax.dot_general(lhs, rhs, NN, preferred_element_type=F32)


def normalize(rows):
    centered = rows - jnp.mean(rows, axis=-1, keepdims=True)
    return centered * lax.rsqrt(jnp.mean(centered * centered, axis=-1, keepdims=True) + LN_EPS)


def head_masks(pair, dim):
    lane = lax.broadcasted_iota(jnp.int32, (1, 256), 1)
    low = 16 * pair
    first = (lane >= low) & (lane < low + dim)
    second = (lane >= low + dim) & (lane < low + 2 * dim)
    return first.astype(BF16), second.astype(BF16)


def inverse_scale(pair, dim, inv_one, inv_two):
    edge = 16 * pair + dim
    lane = lax.broadcasted_iota(jnp.int32, (1, 128), 1)
    if edge < 128:
        return jnp.where(lane < edge, inv_one, inv_two), inv_two
    return inv_one, jnp.where(lane + 128 < edge, inv_one, inv_two)


def store_window(attn, rows, pair, pairs, mixed, scales, high):
    low = mixed[:, :128] * scales[0]
    if high is not None:
        low = low + high
    attn[rows, pl.ds(128 * pair, 128)] = low.astype(BF16)
    high = mixed[:, 128:] * scales[1]
    if pair == pairs - 1:
        attn[rows, pl.ds(128 * pairs, 128)] = high.astype(BF16)
    return high


def spatial_kernel(base_ref, x_ref, mod_ref, wqkv_hbm, wout_hbm, o_ref,
                   wqkv, wout, u, qkv, attn, ks, vs0, vs1, vs2, s0, s1, p0, p1, i0, i1, sem, *, dim):
    tokens, width = u.shape
    vs_slots, s_slots, p_slots, i_slots = (vs0, vs1, vs2), (s0, s1), (p0, p1), (i0, i1)
    first_step = pl.program_id(0) == 0
    video = pl.ds(base_ref[0] + pl.program_id(0), 1)
    starts = list(range(0, width, 256))

    def rows_of(part, c):
        return pl.ds(part * width + starts[c], min(256, width - starts[c]))

    early = [pltpu.make_async_copy(wqkv_hbm.at[rows_of(k, 0)], wqkv.at[rows_of(k, 0)], sem.at[k]) for k in range(3)]
    late = [pltpu.make_async_copy(wqkv_hbm.at[pl.ds(k * width + 256, width - 256)], wqkv.at[pl.ds(k * width + 256, width - 256)], sem.at[3 + k]) for k in range(3)]
    late.append(pltpu.make_async_copy(wout_hbm, wout, sem.at[6]))

    @pl.when(first_step)
    def _():
        for cp in early + late:
            cp.start()

    scale_row = 1.0 + mod_ref[1, video, :]
    shift_row = mod_ref[0, video, :]
    half = tokens // 2

    def modulate(low):
        for i in range(half // 48):
            rows = pl.ds(low + 48 * i, 48)
            u[rows, :] = (normalize(x_ref[0, 0, rows, :].astype(F32)) * scale_row + shift_row).astype(BF16)

    def project(c, rows):
        size = min(256, width - starts[c])
        if size == 256:
            for k in range(3):
                qkv[rows, pl.ds(k * width + starts[c], size)] = dot_nt(u[rows, :], wqkv[rows_of(k, c), :]).astype(BF16)
        else:
            out = dot_nt(u[rows, :], jnp.concatenate([wqkv[rows_of(k, c), :] for k in range(3)], 0)).astype(BF16)
            for k in range(3):
                qkv[rows, pl.ds(k * width + starts[c], size)] = out[:, k * size:(k + 1) * size]

    modulate(0)

    @pl.when(first_step)
    def _():
        for cp in early:
            cp.wait()

    project(0, pl.ds(0, half))
    modulate(half)
    project(0, pl.ds(half, half))

    @pl.when(first_step)
    def _():
        for cp in late:
            cp.wait()

    factor = math.log2(math.e) / math.sqrt(dim)
    pairs = width // (2 * dim)
    main = (tokens // 128) * 128
    lane = lax.broadcasted_iota(jnp.int32, (1, 128), 1)
    in_first = lane < (tokens - main)
    high = None

    def scores(pair):
        first, second = head_masks(pair, dim)
        k_win = qkv[:, pl.ds(width + 128 * pair, 256)]
        v_win = qkv[:, pl.ds(2 * width + 128 * pair, 256)]
        for dst, src in ((ks, k_win), (vs_slots[pair % 3], v_win)):
            one, two = src * first, src * second
            dst[0:main, :] = one[:main]
            dst[main:2 * main, :] = two[:main]
            dst[2 * main:main + tokens, :] = one[main:]
            dst[main + tokens:2 * tokens, :] = two[main:]
        s_slots[pair % 2][...] = dot_nt(qkv[:, pl.ds(128 * pair, 256)], ks[...])

    def probs(pair):
        s_ref, p_ref, i_ref = s_slots[pair % 2], p_slots[pair % 2], i_slots[pair % 2]
        for i in range(tokens // 16):
            rows = pl.ds(16 * i, 16)
            one = s_ref[rows, 0:main]
            two = s_ref[rows, main:2 * main]
            tail = s_ref[rows, 2 * main:2 * tokens]
            max_one, max_two = one[:, :128], two[:, :128]
            for c in range(128, main, 128):
                max_one = jnp.maximum(max_one, one[:, c:c + 128])
                max_two = jnp.maximum(max_two, two[:, c:c + 128])
            max_one = jnp.max(jnp.where(in_first, jnp.maximum(max_one, tail), max_one), -1, keepdims=True) * factor
            max_two = jnp.max(jnp.where(in_first, max_two, jnp.maximum(max_two, tail)), -1, keepdims=True) * factor
            one = jnp.exp2(one * factor - max_one)
            two = jnp.exp2(two * factor - max_two)
            tail = jnp.exp2(tail * factor - jnp.where(in_first, max_one, max_two))
            p_ref[rows, 0:main] = one.astype(BF16)
            p_ref[rows, main:2 * main] = two.astype(BF16)
            p_ref[rows, 2 * main:2 * tokens] = tail.astype(BF16)
            sum_one, sum_two = one[:, :128], two[:, :128]
            for c in range(128, main, 128):
                sum_one = sum_one + one[:, c:c + 128]
                sum_two = sum_two + two[:, c:c + 128]
            sum_one = jnp.sum(sum_one + jnp.where(in_first, tail, 0.0), -1, keepdims=True)
            sum_two = jnp.sum(sum_two + jnp.where(in_first, 0.0, tail), -1, keepdims=True)
            i_ref[rows, 0:128] = jnp.broadcast_to(1.0 / sum_one, (16, 128))
            i_ref[rows, 128:256] = jnp.broadcast_to(1.0 / sum_two, (16, 128))

    for step in range(pairs + 2):
        if step >= 2:
            pair = step - 2
            i_ref = i_slots[pair % 2]
            mixed = dot_nn(p_slots[pair % 2][...], vs_slots[pair % 3][...])
            scales = inverse_scale(pair, dim, i_ref[:, 0:128], i_ref[:, 128:256])
            high = store_window(attn, slice(None), pair, pairs, mixed, scales, high)
        if step < pairs:
            if step % 2 == 1 or step == 0:
                if (step + 1) // 2 + (step == 0) < len(starts):
                    project((step + 1) // 2 + (step == 0), slice(None))
            scores(step)
        if 1 <= step <= pairs:
            probs(step - 1)

    parts, rows_per = o_ref.shape[:2]
    gate = mod_ref[2, video, :]
    branch = dot_nn(attn[...], wout[...])
    x_all = x_ref[0, 0].astype(F32)
    for part in range(parts):
        low = rows_per * part
        o_ref[part] = (x_all[low:low + rows_per] + gate * branch[low:low + rows_per]).astype(BF16)


def temporal_kernel(base_ref, pos_ref, mod_ref, h_hbm, wqkv_hbm, wout_hbm, o_hbm,
                    h_ref, o_ref, wqkv, wout, z, qkv, attn, s0, s1, p0, p1, i0, i1, sem, in_sem, out_sem, *, dim, videos):
    parts, rows, width = h_ref.shape
    s_slots, p_slots, i_slots = (s0, s1), (p0, p1), (i0, i1)
    groups = rows // 16
    group_rows = 16 * parts
    span = 3
    span_rows = span * group_rows
    cuts = (0, 1280, 2560, 3 * width)
    piece = 16 * span

    def rows_copy(src, dst, sems, c):
        at = pl.ds(c * piece, piece)
        return pltpu.make_async_copy(src.at[:, at], dst.at[:, at], sems.at[c])

    loads = [rows_copy(h_hbm, h_ref, in_sem, c) for c in range(groups // span)]
    stores = [rows_copy(o_ref, o_hbm, out_sem, c) for c in range(groups // span)]
    weights = [pltpu.make_async_copy(wqkv_hbm.at[pl.ds(cuts[k], cuts[k + 1] - cuts[k])], wqkv.at[pl.ds(cuts[k], cuts[k + 1] - cuts[k])], sem.at[k]) for k in range(3)]
    weights.append(pltpu.make_async_copy(wout_hbm, wout, sem.at[3]))
    for cp in loads[:1] + weights[:3] + loads[1:] + weights[3:]:
        cp.start()

    def shift(c):
        at = pl.ds(c * piece, piece)
        for part in range(parts):
            shifted = (h_ref[part, at, :].astype(F32) + pos_ref[part:part + 1, :]).astype(BF16)
            for k in range(span):
                z[pl.ds((c * span + k) * group_rows + 16 * part, 16), :] = shifted[16 * k:16 * k + 16]

    loads[0].wait()
    shift(0)

    def project(c, k):
        block = pl.ds(c * span_rows, span_rows)
        qkv[block, cuts[k]:cuts[k + 1]] = dot_nt(z[block, :], wqkv[cuts[k]:cuts[k + 1], :]).astype(BF16)

    for k in range(3):
        weights[k].wait()
        if k == 2:
            for cp in loads[1:] + weights[3:]:
                cp.wait()
        project(0, k)
    for c in range(1, groups // span):
        shift(c)

    factor = math.log2(math.e) / math.sqrt(dim)
    pairs = width // (2 * dim)
    same = (lax.rem(lax.broadcasted_iota(jnp.int32, (16, group_rows), 1), 16)
            == lax.broadcasted_iota(jnp.int32, (16, group_rows), 0))

    def block_of(g):
        return pl.ds(g * group_rows, group_rows)

    def scores(g):
        for pair in range(pairs):
            first, second = head_masks(pair, dim)
            q_win = qkv[block_of(g), pl.ds(128 * pair, 256)]
            k_win = qkv[block_of(g), pl.ds(width + 128 * pair, 256)]
            s_slots[g % 2][pair] = dot_nt(q_win, jnp.concatenate([k_win * first, k_win * second], 0))

    def probs(g):
        for pair in range(pairs):
            for i in range(group_rows // 16):
                at = pl.ds(16 * i, 16)
                for k in range(2):
                    cols = pl.ds(group_rows * k, group_rows)
                    s = jnp.where(same, s_slots[g % 2][pair, at, cols] * factor, -jnp.inf)
                    e = jnp.exp2(s - jnp.max(s, -1, keepdims=True))
                    p_slots[g % 2][pair, at, cols] = e.astype(BF16)
                    i_slots[g % 2][pair, at, cols] = jnp.broadcast_to(1.0 / jnp.sum(e, -1, keepdims=True), (16, group_rows))

    def mix(g):
        high = None
        for pair in range(pairs):
            first, second = head_masks(pair, dim)
            v_win = qkv[block_of(g), pl.ds(2 * width + 128 * pair, 256)]
            mixed = dot_nn(p_slots[g % 2][pair], jnp.concatenate([v_win * first, v_win * second], 0))
            inv = i_slots[g % 2][pair]
            scales = inverse_scale(pair, dim, inv[:, :128], inv[:, 128:])
            high = store_window(attn, block_of(g), pair, pairs, mixed, scales, high)

    per_video = rows // videos

    def finish(c):
        branch = dot_nn(attn[pl.ds(c * span_rows, span_rows), :], wout[...])
        for k in range(span):
            g = c * span + k
            index = lax.broadcasted_iota(jnp.int32, (16, 1), 0) + 16 * g
            gate = mod_ref[2, pl.ds(base_ref[0], 1), :]
            for v in range(1, videos):
                gate = jnp.where(index >= v * per_video, mod_ref[2, pl.ds(base_ref[0] + v, 1), :], gate)
            for part in range(parts):
                base = k * group_rows + 16 * part
                hid = h_ref[part, pl.ds(16 * g, 16), :].astype(F32)
                o_ref[part, pl.ds(16 * g, 16), :] = (hid + gate * branch[base:base + 16]).astype(BF16)

    for step in range(groups + 2):
        if step // span + 1 < groups // span:
            project(step // span + 1, step % span)
        if step >= 2:
            mix(step - 2)
        if step < groups:
            scores(step)
        if 1 <= step <= groups:
            probs(step - 1)
        if step >= 2 and (step - 2) % span == span - 1:
            finish((step - 2) // span)
            stores[(step - 2) // span].start()

    for cp in stores:
        cp.wait()


def text_kernel(base_ref, t_ref, w_ref, o_ref):
    o_ref[...] = dot_nt(t_ref[...], w_ref[...]).astype(BF16)


def cross_mlp_kernel(h_ref, mod_ref, kv_ref, wq_hbm, wo_hbm, win_hbm, wdown_hbm, *refs, dim, aliased, base):
    refs = refs[1:] if aliased else refs
    o_ref, wq, wo, win, wdown, h, q, attn, kpad, hid, s0, s1, p0, p1, i0, i1, sem = refs
    s_slots, p_slots, i_slots = (s0, s1), (p0, p1), (i0, i1)
    tokens, width = h.shape
    parts, rows_per = h_ref.shape[:2]
    text = kv_ref.shape[1]
    first_step = pl.program_id(0) == 0
    video = pl.ds(base + pl.program_id(0), 1)
    copies = [pltpu.make_async_copy(src, dst, sem.at[i]) for i, (src, dst) in
              enumerate(((wq_hbm, wq), (wo_hbm, wo), (win_hbm, win), (wdown_hbm, wdown)))]

    @pl.when(first_step)
    def _():
        for cp in copies:
            cp.start()

    for part in range(parts):
        h[pl.ds(part * rows_per, rows_per), :] = h_ref[part].astype(F32)
    span = kpad.shape[0]
    kpad[text:, :] = jnp.zeros((span - text, 2 * width), BF16)
    kpad[:text, :] = kv_ref[0]

    @pl.when(first_step)
    def _():
        copies[0].wait()
        copies[1].wait()

    q[...] = dot_nt(h[...].astype(BF16), wq[...]).astype(BF16)

    factor = math.log2(math.e) / math.sqrt(dim)
    pairs = width // (2 * dim)
    valid = lax.broadcasted_iota(jnp.int32, (1, 128), 1) < text - (span - 128)
    high = None

    def scores(pair):
        first, second = head_masks(pair, dim)
        k_win = kpad[:, pl.ds(128 * pair, 256)]
        s_slots[pair % 2][...] = dot_nt(q[:, pl.ds(128 * pair, 256)], jnp.concatenate([k_win * first, k_win * second], 0))

    def probs(pair):
        s_ref, p_ref, i_ref = s_slots[pair % 2], p_slots[pair % 2], i_slots[pair % 2]
        for i in range(tokens // 16):
            at = pl.ds(16 * i, 16)
            for k in range(2):
                tiles = [s_ref[at, pl.ds(span * k + c, 128)] * factor for c in range(0, span, 128)]
                tiles[-1] = jnp.where(valid, tiles[-1], -jnp.inf)
                top = jnp.max(functools.reduce(jnp.maximum, tiles), -1, keepdims=True)
                tiles = [jnp.exp2(t - top) for t in tiles]
                for n, t in enumerate(tiles):
                    p_ref[at, pl.ds(span * k + 128 * n, 128)] = t.astype(BF16)
                inv = 1.0 / jnp.sum(sum(tiles[1:], tiles[0]), -1, keepdims=True)
                i_ref[at, pl.ds(128 * k, 128)] = jnp.broadcast_to(inv, (16, 128))

    for step in range(pairs + 2):
        if step >= 2:
            pair = step - 2
            first, second = head_masks(pair, dim)
            i_ref = i_slots[pair % 2]
            v_win = kpad[:, pl.ds(width + 128 * pair, 256)]
            mixed = dot_nn(p_slots[pair % 2][...], jnp.concatenate([v_win * first, v_win * second], 0))
            scales = inverse_scale(pair, dim, i_ref[:, 0:128], i_ref[:, 128:256])
            high = store_window(attn, slice(None), pair, pairs, mixed, scales, high)
        if step < pairs:
            scores(step)
        if 1 <= step <= pairs:
            probs(step - 1)

    scale_row = 1.0 + mod_ref[4, video, :]
    shift_row = mod_ref[3, video, :]
    half = tokens // 2
    for low in (0, half):
        block = pl.ds(low, half)
        h[block, :] = (h[block, :] + dot_nn(attn[block, :], wo[...])).astype(BF16).astype(F32)
        for i in range(half // 48):
            rows = pl.ds(low + 48 * i, 48)
            q[rows, :] = (normalize(h[rows, :]) * scale_row + shift_row).astype(BF16)

    @pl.when(first_step)
    def _():
        copies[2].wait()
        copies[3].wait()

    inner = win.shape[1]
    for low in range(0, inner, 1536):
        cols = pl.ds(low, min(1536, inner - low))
        hid[:, cols] = jax.nn.gelu(dot_nn(q[...], win[:, cols]), approximate=True).astype(BF16)

    o_ref[0, 0] = (h[...] + mod_ref[5, video, :] * dot_nn(hid[...], wdown[...])).astype(BF16)


def any_spec():
    return pl.BlockSpec(memory_space=pl.ANY)


def params():
    return pltpu.CompilerParams(vmem_limit_bytes=VMEM_LIMIT, dimension_semantics=("arbitrary",))


def cost(flops, moved):
    return pl.CostEstimate(flops=flops, transcendentals=0, bytes_accessed=moved)


def spatial_call(latents, modulation, wqkv, wout, base, videos, parts, dim):
    tokens, width = latents.shape[2:]
    rows_per = tokens // parts
    pads = 2 * tokens
    flops = videos * (2 * tokens * width * 4 * width + 4 * tokens * tokens * width)
    return pl.pallas_call(
        functools.partial(spatial_kernel, dim=dim),
        grid_spec=pltpu.PrefetchScalarGridSpec(
            num_scalar_prefetch=1,
            grid=(videos,),
            in_specs=[pl.BlockSpec((1, 1, tokens, width), lambda i, at: (at[0] + i, 0, 0, 0)),
                      pl.BlockSpec(modulation.shape, lambda i, at: (0, 0, 0)),
                      any_spec(), any_spec()],
            out_specs=pl.BlockSpec((parts, rows_per, width), lambda i, at: (0, i, 0)),
            scratch_shapes=[pltpu.VMEM(wqkv.shape, BF16), pltpu.VMEM(wout.shape, BF16),
                        pltpu.VMEM((tokens, width), BF16), pltpu.VMEM((tokens, 3 * width), BF16),
                        pltpu.VMEM((tokens, width), BF16), pltpu.VMEM((pads, 256), BF16)]
        + [pltpu.VMEM((pads, 256), BF16)] * 3 + [pltpu.VMEM((tokens, pads), F32)] * 2
        + [pltpu.VMEM((tokens, pads), BF16)] * 2 + [pltpu.VMEM((tokens, 256), F32)] * 2
        + [pltpu.SemaphoreType.DMA((7,))]),
        out_shape=jax.ShapeDtypeStruct((parts, videos * rows_per, width), BF16),
        compiler_params=params(),
        cost_estimate=cost(flops, 20_000_000),
        name="spatial",
    )(base, latents, modulation, wqkv, wout)


def temporal_call(pos, modulation, pieces, wqkv, wout, base, videos, dim):
    parts, rows, width = pieces.shape
    total = rows * parts
    group_rows = 16 * parts
    pairs = width // (2 * dim)
    flops = 2 * total * width * 4 * width + 4 * total * 256 * width
    return pl.pallas_call(
        functools.partial(temporal_kernel, dim=dim, videos=videos),
        grid_spec=pltpu.PrefetchScalarGridSpec(
            num_scalar_prefetch=1,
            grid=(1,),
            in_specs=[pl.BlockSpec(pos.shape, lambda i, at: (0, 0)),
                      pl.BlockSpec(modulation.shape, lambda i, at: (0, 0, 0)),
                      any_spec(), any_spec(), any_spec()],
            out_specs=any_spec(),
            scratch_shapes=[pltpu.VMEM(pieces.shape, BF16), pltpu.VMEM(pieces.shape, BF16),
                        pltpu.VMEM(wqkv.shape, BF16), pltpu.VMEM(wout.shape, BF16),
                        pltpu.VMEM((total, width), BF16), pltpu.VMEM((total, 3 * width), BF16),
                        pltpu.VMEM((total, width), BF16)]
        + [pltpu.VMEM((pairs, group_rows, 2 * group_rows), F32)] * 2
        + [pltpu.VMEM((pairs, group_rows, 2 * group_rows), BF16)] * 2
        + [pltpu.VMEM((pairs, group_rows, 2 * group_rows), F32)] * 2
        + [pltpu.SemaphoreType.DMA((4,)), pltpu.SemaphoreType.DMA((3,)), pltpu.SemaphoreType.DMA((3,))]),
        out_shape=jax.ShapeDtypeStruct(pieces.shape, BF16),
        compiler_params=params(),
        cost_estimate=cost(flops, 20_000_000),
        name="temporal",
    )(base, pos, modulation, pieces, wqkv, wout)


def text_call(text_ctx, w_kv, base, chunk):
    videos, text, width = text_ctx.shape
    outer = w_kv.shape[0]
    block = 768
    size = chunk * text
    kv = pl.pallas_call(
        text_kernel,
        grid_spec=pltpu.PrefetchScalarGridSpec(
            num_scalar_prefetch=1,
            grid=(outer // block,),
            in_specs=[pl.BlockSpec((size, width), lambda i, at: (at[0] // chunk, 0)),
                      pl.BlockSpec((block, width), lambda i, at: (i, 0))],
            out_specs=pl.BlockSpec((size, block), lambda i, at: (0, i))),
        out_shape=jax.ShapeDtypeStruct((size, outer), BF16),
        compiler_params=params(),
        cost_estimate=cost(2 * size * width * outer, 10_000_000),
        name="text_kv",
    )(base, text_ctx.reshape(videos * text, width), w_kv)
    return kv.reshape(chunk, text, outer)


def cross_mlp_call(pieces, modulation, kv, wq, wo, win, wdown, prev, base, videos, like, dim):
    parts, rows, width = pieces.shape
    text = kv.shape[1]
    inner = win.shape[1]
    rows_per = rows // videos
    tokens = rows_per * parts
    span = ((text + 127) // 128) * 128
    flops = videos * (2 * tokens * width * (2 * width + 2 * inner) + 8 * tokens * span * width)
    aliased = prev is not None
    ins = [pieces, modulation, kv, wq, wo, win, wdown] + ([prev] if aliased else [])
    in_specs = ([pl.BlockSpec((parts, rows_per, width), lambda i: (0, i, 0)),
                 pl.BlockSpec(modulation.shape, lambda i: (0, 0, 0)),
                 pl.BlockSpec((1, text, 2 * width), lambda i: (i, 0, 0))]
                + [any_spec()] * (5 if aliased else 4))
    return pl.pallas_call(
        functools.partial(cross_mlp_kernel, dim=dim, aliased=aliased, base=base),
        grid=(videos,),
        in_specs=in_specs,
        out_specs=pl.BlockSpec((1, 1, tokens, width), lambda i: (base + i, 0, 0, 0)),
        out_shape=jax.ShapeDtypeStruct(like.shape, BF16),
        scratch_shapes=[pltpu.VMEM(wq.shape, BF16), pltpu.VMEM(wo.shape, BF16),
                        pltpu.VMEM(win.shape, BF16), pltpu.VMEM(wdown.shape, BF16),
                        pltpu.VMEM((tokens, width), F32), pltpu.VMEM((tokens, width), BF16),
                        pltpu.VMEM((tokens, width), BF16), pltpu.VMEM((span, 2 * width), BF16),
                        pltpu.VMEM((tokens, inner), BF16)]
        + [pltpu.VMEM((tokens, 2 * span), F32)] * 2 + [pltpu.VMEM((tokens, 2 * span), BF16)] * 2
        + [pltpu.VMEM((tokens, 256), F32)] * 2 + [pltpu.SemaphoreType.DMA((4,))],
        input_output_aliases={len(ins) - 1: 0} if aliased else {},
        compiler_params=params(),
        cost_estimate=cost(flops, 40_000_000),
        name="cross_mlp",
    )(*ins)


CHUNK = 2


def solution(mesh):
    act_spec = P('dp', 'sp', None, None)
    row_spec = P('dp', None, None)
    rep_two = P(None, None)
    rep_three = P(None, None, None)
    rep_four = P(None, None, None, None)
    in_specs = (act_spec, row_spec, row_spec, rep_two, rep_four, rep_three, rep_four, rep_three, rep_three, rep_four, rep_three, rep_two, rep_two)
    parts = mesh.shape['sp']

    def exchange(sent):
        return lax.all_to_all(sent, 'sp', 0, 0, tiled=True)

    def local_block(latents, text_ctx, modulation, pos_temporal, w_qkv_spatial, w_out_spatial, w_qkv_temporal, w_out_temporal, w_query_cross, w_kv_cross, w_out_cross, w_mlp_in, w_mlp_out):
        videos, _, tokens, width = latents.shape
        dim = w_out_spatial.shape[1]
        flat = lambda w: w.reshape(-1, width)
        modulation = jnp.swapaxes(modulation, 0, 1)
        chunks = range(0, videos, CHUNK)
        first = []
        for base in chunks:
            first.append(exchange(spatial_call(latents, modulation, flat(w_qkv_spatial), flat(w_out_spatial), jnp.full((1,), base, jnp.int32), CHUNK, parts, dim)))
        second, kv, backs = [], [], []
        for n, base in enumerate(chunks):
            at = jnp.full((1,), base, jnp.int32)
            back = temporal_call(pos_temporal, modulation, first[n], flat(w_qkv_temporal), flat(w_out_temporal), at, CHUNK, dim)
            _, text_in = lax.optimization_barrier((backs[-1] if backs else first[0], text_ctx))
            back, kv_n = lax.optimization_barrier((back, text_call(text_in, flat(w_kv_cross), at, CHUNK)))
            kv.append(kv_n)
            backs.append(back)
            second.append(exchange(back))
        y = None
        for n, base in enumerate(chunks):
            y = cross_mlp_call(second[n], modulation, kv[n], flat(w_query_cross), flat(w_out_cross), w_mlp_in, w_mlp_out, y, base, CHUNK, latents, dim)
        return y

    return jax.shard_map(local_block, mesh=mesh, in_specs=in_specs, out_specs=act_spec, check_vma=False)
```
